768 devices in a mesh: group: 12 (over z), tensor: 4 (over y_lo), role: 16 (over y_hi, x, core).
Axes of the slice: x: 4, y: 8 (y_hi: 2, y_lo: 4; y = y_hi * 4 + y_lo), z: 12, core: 2. Of those that a mesh axis runs over, the one named last changes fastest.
Arguments:
- tokens: bfloat16 [12, 4096, 2880], P('group', 'role'), may hold values from -6 to 6
- gain: float32 [2880], replicated, may hold values from 0.1 to 1.9
- q_weight: bfloat16 [2880, 2048], P(('group', 'role'), 'tensor'), may hold values from -0.109375 to 0.109375
- kv_weight: bfloat16 [2880, 512], P(('group', 'role'), 'tensor'), may hold values from -0.109375 to 0.109375
- out_weight: bfloat16 [2048, 2880], P('role', 'tensor'), may hold values from -0.5 to 0.5
- sinks: float32 [32], P('tensor'), may hold values from -1 to 3
- segments: int32 [12, 4096], P('group', 'role'), may hold values from 0 to 31, never falling along the last dimension, each value on 1 to 2304 neighbouring positions
Outputs:
- mixed: bfloat16 [12, 4096, 2880], P('group', 'role', 'tensor')
The draws below stay inside these ranges and needn't reach their ends.
Inputs may be any that keep to these rules, and one draw needn't show every extreme that they name: `segments`: within a group, document numbers never fall along the positions; each document holds 1 to 2304 positions and one holds exactly 2304.
All inputs are finite; a program needn't handle non-finite values.
Results may differ from the reference program's by a relative error of at most 0.009.
Values may be sent and summed in bfloat16 or wider, within the bound.
A program may use at most 64 MiB of HBM per device.

```python
import math
import jax
import jax.numpy as jnp
import numpy as np
from jax import lax

D = 2880
HEADS = 32
KV_HEADS = 4
HEAD_DIM = 64
TOK_DEV = 256
SEQ = 4096
DOCS = 32
DOC_MOST = 2304
N_GROUP = 12


def steps_of(rng, shape, shards, smallest, top_value):
    factor_of = 1.0
    for position, blocks in shards:
        draws = jax.random.uniform(jax.random.fold_in(jax.random.fold_in(rng, 6), position), (blocks,), jnp.float32, smallest / len(shards), top_value / len(shards))
        factor_of = factor_of * jnp.repeat(jnp.exp(draws), shape[position] // blocks).reshape((-1,) + (1,) * (len(shape) - 1 - position))
    return factor_of


def length_profile(number_of, total, most, skew):
    portions = [(1 << 20) // math.isqrt(standing ** skew) + 1 for standing in range(2, number_of + 1)]
    surplus, given = total - most - (number_of - 1), [1] * (number_of - 1)
    while surplus > 0:
        candidates = [i for i in range(number_of - 1) if given[i] < most]
        pool, budget = sum([portions[i] for i in candidates]), surplus
        for i in candidates:
            more = min(most - given[i], max(1, budget * portions[i] // pool), surplus)
            given[i] = given[i] + more
            surplus = surplus - more
    return np.array([most] + given)


def ragged_sizes(key, count, total, reach, lean):
    if count == 2:
        one = jax.random.randint(key, (), max(1, total - reach), min(reach, total - 1) + 1)
        return jnp.stack([one, total - one])
    lengths = jnp.asarray(length_profile(count, total, reach, lean), jnp.int32)
    pairs = (count - 1) // 2
    giver, taker = lengths[1:1 + 2 * pairs:2], lengths[2:2 + 2 * pairs:2]
    margin = jnp.minimum(giver - 1, reach - taker)
    moved = jax.random.randint(jax.random.fold_in(key, 1), (pairs,), 0, 1 << 20) % (margin + 1)
    lengths = lengths.at[1:1 + 2 * pairs:2].set(giver - moved).at[2:2 + 2 * pairs:2].set(taker + moved)
    return lengths[jax.random.permutation(jax.random.fold_in(key, 2), count)]


def scatter_about(stream_key, dims, deviation, reach, split=(), kind=jnp.bfloat16):
    level = steps_of(stream_key, dims, split, -0.22, 0.18) if split else 1.0
    entries = jax.random.normal(stream_key, dims, jnp.float32) * deviation * level
    return jnp.minimum(jnp.maximum(entries, -reach), reach).astype(kind)


def setup_inputs(seed: int = 0) -> dict:
    splits = jax.random.split(jax.random.key(seed), 8)
    return {
        "tokens": scatter_about(splits[0], (N_GROUP, SEQ, D), 1.0, 6.0, ((0, 12), (1, 16))),
        "gain": jnp.clip(1.0 + 0.18 * jax.random.normal(splits[1], (D,), jnp.float32), 0.1, 1.9),
        "q_weight": scatter_about(splits[2], (D, HEADS * HEAD_DIM), D ** -0.5, 0.109375, ((0, 192), (1, 4))),
        "kv_weight": scatter_about(splits[3], (D, 2 * KV_HEADS * HEAD_DIM), D ** -0.5, 0.109375, ((0, 192), (1, 4))),
        "out_weight": scatter_about(splits[4], (HEADS * HEAD_DIM, D), (HEADS * HEAD_DIM // 16) ** -0.5, 0.5, ((0, 16), (1, 4))),
        "sinks": jnp.clip(-1.0 + 4.0 * jax.random.uniform(splits[5], (HEADS,), jnp.float32) ** steps_of(splits[5], (HEADS,), ((0, 4),), -0.2, 0.2), -1.0, 3.0),
        "segments": jax.vmap(lambda own: jnp.searchsorted(jnp.cumsum(ragged_sizes(own, DOCS, SEQ, DOC_MOST, 2)), jnp.arange(SEQ), side="right"))(jax.random.split(splits[6], N_GROUP)).reshape((N_GROUP, SEQ)).astype(jnp.int32),
    }


def rotate(vectors, positions):
    half_dim = HEAD_DIM // 2
    frequency = jnp.exp(-jnp.log(150000.0) * jnp.arange(half_dim, dtype=jnp.float32) / half_dim)
    angle = positions[:, None] * frequency[None, :]
    cosine = jnp.cos(angle)[:, None, :]
    sine = jnp.sin(angle)[:, None, :]
    first_half = vectors[..., :half_dim]
    second_half = vectors[..., half_dim:]
    return jnp.concatenate([first_half * cosine - second_half * sine, second_half * cosine + first_half * sine], axis=-1)

def reference(tokens, gain, q_weight, kv_weight, out_weight, sinks, segments):
    group_size = HEADS // KV_HEADS
    positions = jnp.arange(SEQ, dtype=jnp.float32)
    window = DOC_MOST + TOK_DEV
    sink_terms = jnp.exp(sinks).reshape(KV_HEADS, group_size)

    def one_group(inputs):
        feature, doc_ids = inputs
        widened = feature.astype(jnp.float32)
        normed = (widened * lax.rsqrt(lax.optimization_barrier(jnp.mean(widened * widened, axis=-1, keepdims=True)) + 1e-05) * gain).astype(jnp.bfloat16)
        queries = jnp.dot(normed, q_weight, preferred_element_type=jnp.float32).reshape(SEQ, HEADS, HEAD_DIM)
        queries = rotate(queries, positions).astype(jnp.bfloat16)
        paired = jnp.dot(normed, kv_weight, preferred_element_type=jnp.float32).reshape(SEQ, KV_HEADS, 2, HEAD_DIM)
        key_rows = rotate(paired[:, :, 0], positions).astype(jnp.bfloat16)
        value_rows = paired[:, :, 1].astype(jnp.bfloat16)

        def one_block(block_index):
            start = (block_index * TOK_DEV).astype(jnp.int32)
            key_start = jnp.clip(start - DOC_MOST, 0, SEQ - window).astype(jnp.int32)
            query_block = lax.dynamic_slice_in_dim(queries, start, TOK_DEV, 0).reshape(TOK_DEV, KV_HEADS, group_size, HEAD_DIM)
            key_block = lax.dynamic_slice_in_dim(key_rows, key_start, window, 0)
            value_block = lax.dynamic_slice_in_dim(value_rows, key_start, window, 0)
            query_docs = lax.dynamic_slice_in_dim(doc_ids, start, TOK_DEV, 0)
            key_docs = lax.dynamic_slice_in_dim(doc_ids, key_start, window, 0)
            query_pos = start + jnp.arange(TOK_DEV, dtype=jnp.int32)
            key_pos = key_start + jnp.arange(window, dtype=jnp.int32)
            allowed = (key_pos[None, :] <= query_pos[:, None]) & (key_docs[None, :] == query_docs[:, None])
            scores = jnp.einsum('tkgd,nkd->kgtn', query_block.astype(jnp.float32), key_block.astype(jnp.float32)) * 0.125
            weights = jnp.where(allowed[None, None], jnp.exp(scores), 0.0)
            denoms = lax.optimization_barrier(jnp.sum(weights, axis=-1)) + sink_terms[:, :, None]
            rounded = lax.optimization_barrier(weights.astype(jnp.bfloat16))
            summed = jnp.einsum('kgtn,nkd->tkgd', rounded.astype(jnp.float32), value_block.astype(jnp.float32))
            context = summed / jnp.transpose(denoms, (2, 0, 1))[..., None]
            return context.astype(jnp.bfloat16).reshape(TOK_DEV, HEADS * HEAD_DIM)
        context = lax.map(one_block, jnp.arange(SEQ // TOK_DEV, dtype=jnp.int32)).reshape(SEQ, HEADS * HEAD_DIM)
        return jnp.dot(context, out_weight, preferred_element_type=jnp.float32).astype(jnp.bfloat16)
    return lax.map(one_group, (tokens, segments))
```

```python
import functools
import math

import jax
import jax.numpy as jnp
import numpy as np
from jax import lax
from jax.experimental import pallas as pl
from jax.experimental.pallas import tpu as pltpu
from jax.sharding import PartitionSpec as P

HEAD_DIM = 64
REACH = 9
CHUNKS = 4
NEG = -1e30
LOG2E = 1.4426950408889634
F32 = jnp.float32
BF16 = jnp.bfloat16


def kernel(
    dims,
    tokens,
    gain,
    w_in,
    wo_in,
    seg_rows,
    seg_cols,
    sink_exp,
    near_cos,
    near_sin,
    far_cos,
    far_sin,
    out,
    normed,
    spread,
    w_all,
    acc,
    q_all,
    kv_all,
    bias,
    o_acc,
    wo_all,
    ctx,
    out_acc,
    plane_send,
    plane_recv,
    ring_send,
    ring_recv,
    twin_send,
    twin_recv,
    ctx_send,
    ctx_recv,
):
    NG, NT, R, NX, ROWS, D = dims
    HALF = R // 2
    H = NG // 2
    PAIRS = q_all.shape[0] // 2
    WIDE = q_all.shape[0] * HEAD_DIM
    PER = HALF // CHUNKS
    g = lax.axis_index("group")
    t = lax.axis_index("tensor")
    r = lax.axis_index("role")
    c = lax.rem(r, 2)
    x = lax.rem(r // 2, NX)
    yh = r // HALF

    def role_of(y_, x_, c_):
        return y_ * HALF + x_ * 2 + c_

    def x_at(dx):
        return lax.rem(x + dx, NX)

    twin = {"role": role_of(yh, x, 1 - c)}
    across = {"role": role_of(1 - yh, x, c)}

    def x_to(dx):
        return {"role": role_of(yh, x_at(dx), c)}

    up = lax.rem(g + 1, NG)
    down = lax.rem(g + NG - 1, NG)

    def remote(src, dst, send, recv, where):
        return pltpu.make_async_remote_copy(
            src_ref=src,
            dst_ref=dst,
            send_sem=send,
            recv_sem=recv,
            device_id=where,
            device_id_type=pl.DeviceIdType.MESH,
        )

    greeted = [twin, across, {"group": up}, {"group": down}]
    greeted += [x_to(dx) for dx in range(1, NX)]
    greeted += [{"tensor": lax.rem(t + dt, NT)} for dt in range(1, NT)]
    barrier = pltpu.get_barrier_semaphore()
    for where in greeted:
        pl.semaphore_signal(
            barrier, inc=1, device_id=where, device_id_type=pl.DeviceIdType.MESH
        )
    pl.semaphore_wait(barrier, len(greeted))

    class Gather:
        def __init__(self, which, own, slot):
            self.send = plane_send.at[which]
            self.recv = plane_recv.at[which]
            self.own = own
            self.slot = slot

        def copy(self, index, role, where, src=None):
            dst = self.slot(role)
            return remote(
                dst if src is None else src, dst, self.send.at[index], self.recv.at[index], where
            )

        def across(self):
            return self.copy(0, r, across, self.own)

        def along(self, dx):
            return self.copy(dx, r, x_to(dx), self.own)

        def along_other(self, dx):
            return self.copy(NX - 1 + dx, role_of(1 - yh, x, c), x_to(dx))

        def twin_near(self, dx):
            if dx == 0:
                return self.copy(2 * NX, r, twin, self.own)
            return self.copy(2 * NX + dx, role_of(yh, lax.rem(x + NX - dx, NX), c), twin)

        def twin_other(self, dx):
            return self.copy(3 * NX + dx, role_of(1 - yh, lax.rem(x + NX - dx, NX), c), twin)

    gather_w = Gather(
        0,
        w_in,
        lambda role: w_all.at[
            g, lax.rem(role, 2) * HALF + (role // HALF) * NX + lax.rem(role // 2, NX)
        ],
    )
    gather_o = Gather(1, wo_in, lambda role: wo_all.at[role])
    gather_k = Gather(2, kv_all.at[r], lambda role: kv_all.at[role])
    offsets = range(1, NX)

    gather_w.across().start()
    for dx in offsets:
        gather_w.along(dx).start()
    gather_w.twin_near(0).start()
    own_slot = c * HALF + yh * NX + x
    w_all[g, own_slot] = w_in[...]
    wo_all[r] = wo_in[...]

    top = (D // 128) * 128
    if normed.shape[1] > top:
        normed[:, top:] = jnp.zeros((ROWS, normed.shape[1] - top), BF16)

    def norm_rows(i, _):
        rows = pl.ds(pl.multiple_of(i * 16, 16), 16)
        wide = tokens[rows, :].astype(F32)
        scale = lax.rsqrt(jnp.sum(wide * wide, axis=-1, keepdims=True) * (1.0 / D) + 1e-05)
        normed[rows, 0:D] = (wide * scale * gain[...]).astype(BF16)
        return 0

    lax.fori_loop(0, ROWS // 16, norm_rows, 0)

    for dx in offsets:
        gather_w.along(dx).wait_recv()
        gather_w.twin_near(dx).start()

    window = spread_window(R)
    lane = lax.broadcasted_iota(jnp.int32, (1, R * 16), 1)
    slot_of = lane // 16
    within = lax.rem(lane, 16)
    slot_role = (
        (lax.rem(slot_of, HALF) // NX) * HALF + lax.rem(slot_of, NX) * 2 + slot_of // HALF
    )
    feature = jnp.where(within < 15, slot_role * 15 + within, -4096)
    row_id = lax.broadcasted_iota(jnp.int32, (window, R * 16), 0)

    def spread_plane(p, _):
        first = p * (15 * R)
        start = (first // 128) * 128
        hit = row_id == (feature + (first - start))
        pick = jnp.where(hit, 1.0, 0.0).astype(BF16)
        part = normed[:, pl.ds(pl.multiple_of(start, 128), window)]
        spread[p] = jnp.dot(part, pick, preferred_element_type=F32).astype(BF16)
        return 0

    lax.fori_loop(0, NG, spread_plane, 0)

    gather_w.across().wait_recv()
    for dx in offsets:
        gather_w.along_other(dx).start()
    gather_w.twin_other(0).start()
    for dx in offsets:
        gather_w.along_other(dx).wait_recv()

    def plane(d, s):
        return lax.rem(g - s + NG, NG) if d == 0 else lax.rem(g + s, NG)

    def ring(d, s, j):
        ref = w_all.at[plane(d, s), pl.ds(c * HALF + j * PER, PER)]
        return remote(
            ref,
            ref,
            ring_send.at[d, s, j],
            ring_recv.at[d, s, j],
            {"group": up if d == 0 else down},
        )

    def twin_plane(d, s):
        ref = w_all.at[plane(d, s), pl.ds(c * HALF, HALF)]
        return remote(ref, ref, twin_send.at[d, s], twin_recv.at[d, s], twin)

    def twin_half(d):
        ref = w_all.at[plane(d, H), pl.ds(c * HALF + d * (HALF // 2), HALF // 2)]
        return remote(ref, ref, twin_send.at[d, H], twin_recv.at[d, H], twin)

    def last_chunks(d):
        return range(d * (CHUNKS // 2), (d + 1) * (CHUNKS // 2))

    def add_plane(p):
        acc[...] += jnp.dot(
            spread[p],
            w_all[p].reshape(R * 16, acc.shape[1]),
            preferred_element_type=F32,
        )

    for j in range(CHUNKS):
        for d in range(2):
            ring(d, 0, j).start()
    for dx in offsets:
        gather_w.twin_other(dx).start()
    gather_o.across().start()
    for dx in offsets:
        gather_o.along(dx).start()
    gather_o.twin_near(0).start()

    for dx in range(NX):
        gather_w.twin_near(dx).wait_recv()
        gather_w.twin_other(dx).wait_recv()
    acc[...] = jnp.zeros_like(acc)
    add_plane(g)

    def turn(s, _):
        for j in range(CHUNKS):
            for d in range(2):
                ring(d, s - 1, j).wait_recv()
                ring(d, s, j).start()
        for d in range(2):
            twin_plane(d, s).start()

        @pl.when(s >= 2)
        def _():
            for d in range(2):
                twin_plane(d, s - 1).wait_recv()
                add_plane(plane(d, s - 1))

        return 0

    if H > 2:
        lax.fori_loop(1, H - 1, turn, 0)
    for j in range(CHUNKS):
        for d in range(2):
            ring(d, H - 2, j).wait_recv()
            if j in last_chunks(d):
                ring(d, H - 1, j).start()
    for d in range(2):
        twin_plane(d, H - 1).start()
    if H > 2:
        for d in range(2):
            twin_plane(d, H - 2).wait_recv()
            add_plane(plane(d, H - 2))
    for d in range(2):
        twin_plane(d, H - 1).wait_recv()
        add_plane(plane(d, H - 1))
    for d in range(2):
        for j in last_chunks(d):
            ring(d, H - 1, j).wait_recv()
        twin_half(d).start()
    for d in range(2):
        twin_half(d).wait_recv()
    add_plane(plane(0, H))

    cos_far = far_cos[pl.ds(r, 1), :]
    sin_far = far_sin[pl.ds(r, 1), :]
    cos = near_cos[...] * cos_far - near_sin[...] * sin_far
    sin = near_sin[...] * cos_far + near_cos[...] * sin_far
    lanes = lax.broadcasted_iota(jnp.int32, (ROWS, 128), 1)
    first_half = lax.rem(lanes, HEAD_DIM) < HEAD_DIM // 2
    low = lanes < HEAD_DIM
    signed = jnp.where(first_half, -sin, sin)

    def swapped(u):
        return jnp.where(
            first_half, pltpu.roll(u, 128 - HEAD_DIM // 2, 1), pltpu.roll(u, HEAD_DIM // 2, 1)
        )

    pair = acc[:, WIDE : WIDE + 128]
    turned = pair * jnp.where(low, cos, 1.0) + swapped(pair) * jnp.where(low, signed, 0.0)
    kv_all[r, 0:ROWS] = turned.astype(BF16)
    kv_all[r, ROWS : ROWS + 16] = seg_rows[...]

    @pl.when(yh == 0)
    def _():
        gather_k.across().start()

    for dx in offsets:
        gather_k.along(dx).start()
    gather_k.twin_near(0).start()

    fold = 0.125 * LOG2E
    for i in range(PAIRS):
        u = acc[:, 128 * i : 128 * (i + 1)]
        turned = (u * cos + swapped(u) * signed) * fold
        q_all[2 * i] = jnp.where(low, turned, 0.0).astype(BF16)
        q_all[2 * i + 1] = jnp.where(low, pltpu.roll(turned, HEAD_DIM, 1), 0.0).astype(BF16)

    q_pos = lax.broadcasted_iota(jnp.int32, (ROWS, 128), 0) + r * ROWS
    k_off = lax.broadcasted_iota(jnp.int32, (ROWS, 128), 1)

    def make_bias(b):
        docs = seg_cols[...].astype(F32)
        for part in range(ROWS // 128):
            keys = kv_all[b, ROWS + part : ROWS + part + 1, :].astype(F32)
            seen = (docs == keys) & (k_off + (b * ROWS + part * 128) <= q_pos)
            bias[b, :, part * 128 : (part + 1) * 128] = jnp.where(seen, 0.0, NEG)

    def attend(b, h, fresh=False):
        block = kv_all[b, 0:ROWS, :]
        scores = lax.dot_general(
            q_all[h], block, (((1,), (1,)), ((), ())), preferred_element_type=F32
        )
        weights = jnp.exp2(scores + bias[b]).astype(BF16)
        lanes_b = lax.broadcasted_iota(jnp.int32, block.shape, 1)
        with_ones = jnp.where(lanes_b < HEAD_DIM, jnp.ones_like(block), block)
        added = jnp.dot(weights, with_ones, preferred_element_type=F32)
        if fresh:
            o_acc[h] = added
        else:
            o_acc[h] += added

    make_bias(r)

    def own_pair(i, _):
        attend(r, 2 * i, True)
        attend(r, 2 * i + 1, True)
        return 0

    lax.fori_loop(0, PAIRS, own_pair, 0)

    for dx in offsets:
        gather_k.along(dx).wait_recv()
        gather_k.twin_near(dx).start()

    @pl.when(yh == 1)
    def _():
        gather_k.across().wait_recv()
        for dx in offsets:
            gather_k.along_other(dx).start()
        gather_k.twin_other(0).start()

    for dx in range(NX):
        gather_k.twin_near(dx).wait_recv()

    def near_block(b, _):
        make_bias(b)

        def of_pair(i, _):
            attend(b, 2 * i)
            attend(b, 2 * i + 1)
            return 0

        lax.fori_loop(0, PAIRS, of_pair, 0)
        return 0

    lax.fori_loop(yh * HALF, r, near_block, 0)

    @pl.when(yh == 1)
    def _():
        for dx in offsets:
            gather_k.along_other(dx).wait_recv()
            gather_k.twin_other(dx).start()

    for dx in offsets:
        gather_o.along(dx).wait_recv()
        gather_o.twin_near(dx).start()
    gather_o.across().wait_recv()
    for dx in offsets:
        gather_o.along_other(dx).start()
    gather_o.twin_other(0).start()

    far_from = jnp.maximum(r - REACH, 0)
    far_to = jnp.where(yh == 1, HALF, far_from)

    @pl.when(yh == 1)
    def _():
        for dx in range(NX):
            gather_k.twin_other(dx).wait_recv()

        def far_bias(b, _):
            make_bias(b)
            return 0

        lax.fori_loop(far_from, HALF, far_bias, 0)

    def ctx_copy(i, dt):
        ref = ctx.at[t, i]
        return remote(
            ref, ref, ctx_send.at[i, dt], ctx_recv.at[i, dt], {"tensor": lax.rem(t + dt, NT)}
        )

    def finish_pair(i, _):
        def far_block(b, _):
            attend(b, 2 * i)
            attend(b, 2 * i + 1)
            return 0

        lax.fori_loop(far_from, far_to, far_block, 0)
        even = o_acc[2 * i]
        odd = o_acc[2 * i + 1]
        even = pltpu.roll(even, HEAD_DIM, 1) / (even + sink_exp[pl.ds(2 * i, 1), :])
        odd = odd / (pltpu.roll(odd, HEAD_DIM, 1) + sink_exp[pl.ds(2 * i + 1, 1), :])
        ctx[t, i] = jnp.where(low, even, odd).astype(BF16)
        for dt in range(1, NT):
            ctx_copy(i, dt).start()
        return 0

    lax.fori_loop(0, PAIRS, finish_pair, 0)

    for dx in offsets:
        gather_o.along_other(dx).wait_recv()
        gather_o.twin_other(dx).start()
    for dx in range(NX):
        gather_o.twin_near(dx).wait_recv()
        gather_o.twin_other(dx).wait_recv()

    def project(tt):
        heads = jnp.concatenate([ctx[tt, i] for i in range(PAIRS)], axis=1)
        rows = wo_all[pl.ds(tt * (R // NT), R // NT)].reshape(WIDE, out.shape[1])
        return jnp.dot(heads, rows, preferred_element_type=F32)

    out_acc[...] = project(t)
    for dt in range(1, NT):
        for i in range(PAIRS):
            ctx_copy(i, dt).wait_recv()
        out_acc[...] += project(lax.rem(t + NT - dt, NT))
    out[...] = out_acc[...].astype(BF16)

    for gather in (gather_w, gather_o):
        gather.across().wait_send()
        for dx in offsets:
            gather.along(dx).wait_send()
            gather.along_other(dx).wait_send()
        for dx in range(NX):
            gather.twin_near(dx).wait_send()
            gather.twin_other(dx).wait_send()

    @pl.when(yh == 0)
    def _():
        gather_k.across().wait_send()

    for dx in offsets:
        gather_k.along(dx).wait_send()
    for dx in range(NX):
        gather_k.twin_near(dx).wait_send()

    @pl.when(yh == 1)
    def _():
        for dx in offsets:
            gather_k.along_other(dx).wait_send()
        for dx in range(NX):
            gather_k.twin_other(dx).wait_send()

    def sent(s, _):
        for d in range(2):
            for j in range(CHUNKS):
                ring(d, s, j).wait_send()

            @pl.when(s >= 1)
            def _():
                twin_plane(d, s).wait_send()

        return 0

    lax.fori_loop(0, H - 1, sent, 0)
    for d in range(2):
        twin_plane(d, H - 1).wait_send()
        for j in last_chunks(d):
            ring(d, H - 1, j).wait_send()
        twin_half(d).wait_send()

    def ctx_sent(i, _):
        for dt in range(1, NT):
            ctx_copy(i, dt).wait_send()
        return 0

    lax.fori_loop(0, PAIRS, ctx_sent, 0)


def spread_window(R):
    return -(-(15 * R + 127) // 128) * 128


def rotation_tables(rows, roles):
    half = HEAD_DIM // 2
    freq = np.exp(-math.log(150000.0) * np.arange(half) / half)
    freq = np.tile(freq, 128 // half)[None, :]
    near = np.arange(rows)[:, None] * freq
    far = (np.arange(roles) * rows)[:, None] * freq
    return [a.astype(np.float32) for a in (np.cos(near), np.sin(near), np.cos(far), np.sin(far))]


def on_device(sizes, tokens, gain, q_weight, kv_weight, out_weight, sinks, segments):
    NG, NT, R = sizes
    feature = tokens[0]
    docs = segments[0]
    rows, width = feature.shape
    NX = R // 4
    heads = q_weight.shape[1] // HEAD_DIM
    features_out = out_weight.shape[1]
    both = jnp.concatenate([q_weight, kv_weight], axis=1)
    w_in = jnp.pad(both, ((0, 1), (0, 0)))
    seg_rows = jnp.pad(docs.astype(BF16).reshape(rows // 128, 128), ((0, 16 - rows // 128), (0, 0)))
    seg_cols = jnp.broadcast_to(docs.astype(BF16)[:, None], (rows, 128))
    sink_exp = jnp.broadcast_to(jnp.exp(sinks)[:, None], (heads, 128))
    tables = [jnp.asarray(a) for a in rotation_tables(rows, R)]
    window = spread_window(R)
    norm_width = ((NG - 1) * 15 * R // 128) * 128 + window
    H = NG // 2
    dims = (NG, NT, R, NX, rows, width)
    vmem = pl.BlockSpec(memory_space=pltpu.VMEM)
    dma = pltpu.SemaphoreType.DMA
    out = pl.pallas_call(
        functools.partial(kernel, dims),
        out_shape=jax.ShapeDtypeStruct((rows, features_out), BF16),
        in_specs=[vmem] * 11,
        out_specs=vmem,
        scratch_shapes=[
            pltpu.VMEM((rows, norm_width), BF16),
            pltpu.VMEM((NG, rows, R * 16), BF16),
            pltpu.VMEM((NG, R, 16, both.shape[1]), BF16),
            pltpu.VMEM((rows, both.shape[1]), F32),
            pltpu.VMEM((heads, rows, 128), BF16),
            pltpu.VMEM((R, rows + 16, 128), BF16),
            pltpu.VMEM((R, rows, rows), F32),
            pltpu.VMEM((heads, rows, 128), F32),
            pltpu.VMEM((R, out_weight.shape[0], features_out), BF16),
            pltpu.VMEM((NT, heads // 2, rows, 128), BF16),
            pltpu.VMEM((rows, features_out), F32),
            dma((3, 4 * NX)),
            dma((3, 4 * NX)),
            dma((2, H, CHUNKS)),
            dma((2, H, CHUNKS)),
            dma((2, H + 1)),
            dma((2, H + 1)),
            dma((heads // 2, NT)),
            dma((heads // 2, NT)),
        ],
        compiler_params=pltpu.CompilerParams(collective_id=0, has_side_effects=True),
        name="layer",
    )(feature, gain[None], w_in, out_weight, seg_rows, seg_cols, sink_exp, *tables)
    return out[None]


def solution(mesh):
    placed = (
        P("group", "role", None),
        P(),
        P(("group", "role"), "tensor"),
        P(("group", "role"), "tensor"),
        P("role", "tensor"),
        P("tensor"),
        P("group", "role"),
    )
    sizes = (mesh.shape["group"], mesh.shape["tensor"], mesh.shape["role"])
    return jax.shard_map(
        functools.partial(on_device, sizes),
        mesh=mesh,
        in_specs=placed,
        out_specs=P("group", "role", "tensor"),
        check_vma=False,
    )
```

```python
import functools
import math

import jax
import jax.numpy as jnp
import numpy as np
from jax import lax
from jax.experimental import pallas as pl
from jax.experimental.pallas import tpu as pltpu
from jax.sharding import PartitionSpec as P

HEAD_DIM = 64
REACH = 9
NEG = -1e30
LOG2E = 1.4426950408889634
F32 = jnp.float32
BF16 = jnp.bfloat16


def kernel(
    dims,
    tokens_hbm,
    gain,
    wq_in,
    wkv_in,
    wo_hbm,
    docs_in,
    sinks,
    near_cos,
    near_sin,
    far_cos,
    far_sin,
    out,
    tokens,
    normed,
    spread,
    w_own,
    w_all,
    acc,
    q_all,
    kv_all,
    v_all,
    docs_col,
    bias,
    o_acc,
    wo_all,
    ctx,
    out_acc,
    load_sem,
    plane_send,
    plane_recv,
    ring_send,
    ring_recv,
    side_send,
    side_recv,
    twin_send,
    twin_recv,
    ctx_send,
    ctx_recv,
    pass_send,
):
    NG, NT, R, NX, ROWS, D = dims
    HALF = R // 2
    H = NG // 2
    PAIRS = q_all.shape[0] // 2
    WIDE = q_all.shape[0] * HEAD_DIM
    g = lax.axis_index("group")
    t = lax.axis_index("tensor")
    r = lax.axis_index("role")
    c = lax.rem(r, 2)
    x = lax.rem(r // 2, NX)
    yh = r // HALF

    def role_of(y_, x_, c_):
        return y_ * HALF + x_ * 2 + c_

    def x_at(dx):
        return lax.rem(x + dx, NX)

    twin = {"role": role_of(yh, x, 1 - c)}
    across = {"role": role_of(1 - yh, x, c)}

    beyond = {"role": role_of(1 - yh, x_at(NX // 2), c)}

    def x_to(dx):
        return {"role": role_of(yh, x_at(dx), c)}

    up = lax.rem(g + 1, NG)
    down = lax.rem(g + NG - 1, NG)

    def remote(src, dst, send, recv, where):
        return pltpu.make_async_remote_copy(
            src_ref=src,
            dst_ref=dst,
            send_sem=send,
            recv_sem=recv,
            device_id=where,
            device_id_type=pl.DeviceIdType.MESH,
        )

    load_tokens = pltpu.make_async_copy(tokens_hbm, tokens, load_sem.at[0])
    load_tokens.start()
    load_wo = pltpu.make_async_copy(wo_hbm, wo_all.at[r], load_sem.at[1])
    load_wo.start()
    w_own[0:15, 0:WIDE] = wq_in[...]
    w_own[0:15, WIDE : WIDE + 128] = wkv_in[...]
    w_own[15:16, :] = jnp.zeros((1, WIDE + 128), BF16)

    greeted = [twin, across, {"group": up}, {"group": down}]
    greeted += [x_to(dx) for dx in range(1, NX)]
    if NX > 2:
        greeted += [beyond]
    greeted += [{"tensor": lax.rem(t + dt, NT)} for dt in range(1, NT)]
    barrier = pltpu.get_barrier_semaphore()
    for where in greeted:
        pl.semaphore_signal(
            barrier, inc=1, device_id=where, device_id_type=pl.DeviceIdType.MESH
        )
    pl.semaphore_wait(barrier, len(greeted))

    class Gather:
        def __init__(self, which, own, slot):
            self.send = plane_send.at[which]
            self.recv = plane_recv.at[which]
            self.own = own
            self.slot = slot

        def copy(self, index, role, where, src=None):
            dst = self.slot(role)
            return remote(
                dst if src is None else src, dst, self.send.at[index], self.recv.at[index], where
            )

        def across(self):
            return self.copy(0, r, across, self.own)

        def along(self, dx):
            return self.copy(dx, r, x_to(dx), self.own)

        def along_other(self, dx):
            return self.copy(NX - 1 + dx, role_of(1 - yh, x, c), x_to(dx))

        def twin_near(self, dx):
            if dx == 0:
                return self.copy(2 * NX, r, twin, self.own)
            return self.copy(2 * NX + dx, role_of(yh, lax.rem(x + NX - dx, NX), c), twin)

        def twin_other(self, dx):
            return self.copy(3 * NX + dx, role_of(1 - yh, lax.rem(x + NX - dx, NX), c), twin)

    gather_k = Gather(2, kv_all.at[r], lambda role: kv_all.at[role])
    offsets = range(1, NX)

    far = [2] if NX > 2 else []
    near = [1, NX - 1] if NX > 2 else [1]
    upper = (wo_all.shape[1] // 2) // 16 * 16

    def own_block(slot):
        return w_all.at[g, c * HALF + slot]

    def w_copy(index, slot, where):
        return remote(
            w_own, own_block(slot), plane_send.at[0, index], plane_recv.at[0, index], where
        )

    w_across = w_copy(0, NX, across)
    w_far = [w_copy(1, dx, x_to(dx)) for dx in far]
    w_beyond = [w_copy(2, NX + dx, beyond) for dx in far]
    travels = {0: 0, NX: 2}
    for dx in far:
        travels.update({dx: 1, NX + dx: 2})

    def plane(d, s):
        return lax.rem(g - s + NG, NG) if d == 0 else lax.rem(g + s, NG)

    def ring(d, s, j):
        dst = w_all.at[plane(d, s), c * HALF + j]
        return remote(
            w_own if s == 0 and j == 0 else dst,
            dst,
            ring_send.at[d, s, j],
            ring_recv.at[d, s, j],
            {"group": up if d == 0 else down},
        )

    def side(d, s, j, i):
        slot = c * HALF + j
        index = (d, s, 2 * (j // NX) + i)
        return remote(
            w_own if s == 0 and j == 0 else w_all.at[plane(d, s), slot],
            w_all.at[plane(d, s), slot + near[i]],
            side_send.at[index],
            side_recv.at[index],
            x_to(near[i]),
        )

    def sides(d, s):
        return [side(d, s, j, i) for j in (0, NX) for i in range(len(near))]

    def both(s):
        return range(2 if 0 < s < H else 1)

    def o_copy(index, role, where, rows=None):
        ref = wo_all.at[role] if rows is None else wo_all.at[role, rows]
        return remote(ref, ref, plane_send.at[1, index], plane_recv.at[1, index], where)

    def behind(y_, dx):
        return role_of(y_, lax.rem(x + NX - dx, NX), c)

    def halves():
        return (pl.ds(0, upper), pl.ds(upper, wo_all.shape[1] - upper))

    o_across = o_copy(0, r, across)

    def o_side(dy, i):
        return o_copy(1 + 4 * dy + i, behind(yh if dy == 0 else 1 - yh, 0), x_to(near[i]))

    def o_on(dy, i):
        role = behind(yh if dy == 0 else 1 - yh, near[i])
        return o_copy(3 + 4 * dy + i, role, x_to(near[i]), halves()[i])

    def o_twin(dy, dx):
        return o_copy(9 + dy * NX + dx, behind(yh if dy == 0 else 1 - yh, dx), twin)

    def o_take_sides(dy):
        for i in range(len(near)):
            o_side(dy, i).wait_recv()
            if far:
                o_on(dy, i).start()
            o_twin(dy, near[i]).start()

    def o_take_far(dy):
        for dx in far:
            for i in range(2):
                o_on(dy, i).wait_recv()
            o_twin(dy, dx).start()

    def twin_plane(d, s):
        ref = w_all.at[plane(d, s), pl.ds(c * HALF, HALF)]
        return remote(ref, ref, twin_send.at[d, s], twin_recv.at[d, s], twin)

    def last(j):
        return j // NX

    def add_plane(p):
        acc[...] += jnp.dot(
            spread[p],
            w_all[p].reshape(R * 16, acc.shape[1]),
            preferred_element_type=F32,
        )

    def round_of_ring(n):
        for j, delay in travels.items():
            s = n - delay
            if s < 0 or s > H:
                continue
            if s == 0 and j == NX:
                w_across.wait_recv()
            elif s == 0 and j > NX:
                w_beyond[0].wait_recv()
            elif s == 0 and j > 0:
                w_far[0].wait_recv()
            for d in range(2):
                if 1 <= s < H or (s == H and d == last(j)):
                    ring(d, s - 1, j).wait_recv()
                if s < H - 1 or (s == H - 1 and d == last(j)):
                    ring(d, s, j).start()
            if j % NX == 0:
                for d in both(s):
                    for i in range(len(near)):
                        side(d, s, j, i).start()
        whole = n - 3
        if whole >= 0:
            for d in both(whole):
                for copy in sides(d, whole):
                    copy.wait_recv()
                twin_plane(d, whole).start()

    def add_planes(s):
        for d in both(s):
            twin_plane(d, s).wait_recv()
            add_plane(plane(d, s))

    w_across.start()
    for copy in w_beyond + w_far:
        copy.start()
    round_of_ring(0)
    w_all[g, c * HALF] = w_own[...]
    load_wo.wait()
    o_across.start()
    for i in range(len(near)):
        o_side(0, i).start()
    o_twin(0, 0).start()

    load_tokens.wait()

    def add_squares(i, total):
        wide = tokens[pl.ds(pl.multiple_of(i * 160, 32), 160), :].astype(F32)
        return total + jnp.sum((wide * wide).reshape(20, 8, ROWS), axis=0)

    squares = lax.fori_loop(0, D // 160, add_squares, jnp.zeros((8, ROWS), F32))
    scale = lax.rsqrt(jnp.sum(squares, axis=0, keepdims=True) * (1.0 / D) + 1e-05)

    def norm_rows(start, count):
        row = jnp.broadcast_to(gain[pl.ds(start, count)][None], (128, count))
        column = jnp.transpose(row)
        wide = tokens[pl.ds(start, count), :].astype(F32)
        normed[pl.ds(start, count), :] = (
            wide * scale * jnp.concatenate([column] * (ROWS // 128), axis=1)
        ).astype(BF16)

    def norm_full(i, _):
        norm_rows(pl.multiple_of(i * 128, 128), 128)
        return 0

    lax.fori_loop(0, D // 128, norm_full, 0)
    if D % 128:
        norm_rows(D // 128 * 128, D % 128)
    round_of_ring(1)
    round_of_ring(2)
    lane = lax.broadcasted_iota(jnp.int32, (15 * R, R * 16), 1)
    slot_of = lane // 16
    within = lax.rem(lane, 16)
    rel = lax.rem(slot_of, HALF)
    slot_role = role_of(
        lax.rem(yh + rel // NX, 2), lax.rem(x + NX - lax.rem(rel, NX), NX), slot_of // HALF
    )
    feature = jnp.where(within < 15, slot_role * 15 + within, -1)
    hit = lax.broadcasted_iota(jnp.int32, (15 * R, R * 16), 0) == feature
    pick = jnp.where(hit, 1.0, 0.0).astype(BF16)

    def spread_plane(p, _):
        part = normed[pl.ds(pl.multiple_of(p * (15 * R), 8), 15 * R), :]
        spread[p] = lax.dot_general(
            part, pick, (((0,), (0,)), ((), ())), preferred_element_type=F32
        ).astype(BF16)
        return 0

    lax.fori_loop(0, NG, spread_plane, 0)
    acc[...] = jnp.zeros_like(acc)
    docs = docs_in[...].astype(F32)
    for part in range(ROWS // 128):
        row = jnp.broadcast_to(docs[:, 128 * part : 128 * (part + 1)], (128, 128))
        docs_col[128 * part : 128 * (part + 1), :] = jnp.transpose(row)
    round_of_ring(3)
    for n in range(4, H + 4):
        round_of_ring(n)
        add_planes(n - 4)
        if n == 5:
            o_take_sides(0)
    add_planes(H)

    cos_far = far_cos[pl.ds(r, 1), :]
    sin_far = far_sin[pl.ds(r, 1), :]
    cos = near_cos[...] * cos_far - near_sin[...] * sin_far
    sin = near_sin[...] * cos_far + near_cos[...] * sin_far
    lanes = lax.broadcasted_iota(jnp.int32, (ROWS, 128), 1)
    first_half = lax.rem(lanes, HEAD_DIM) < HEAD_DIM // 2
    low = lanes < HEAD_DIM
    signed = jnp.where(first_half, -sin, sin)

    def swapped(u):
        return jnp.where(
            first_half, pltpu.roll(u, 128 - HEAD_DIM // 2, 1), pltpu.roll(u, HEAD_DIM // 2, 1)
        )

    pair = acc[:, WIDE : WIDE + 128]
    turned = pair * jnp.where(low, cos, 1.0) + swapped(pair) * jnp.where(low, signed, 0.0)
    kv_all[r, 0:ROWS] = turned.astype(BF16)
    doc_rows = jnp.zeros((16, 128), F32)
    line = lax.broadcasted_iota(jnp.int32, (16, 128), 0)
    for part in range(ROWS // 128):
        doc_rows = jnp.where(line == part, docs[:, 128 * part : 128 * (part + 1)], doc_rows)
    kv_all[r, ROWS : ROWS + 16] = doc_rows.astype(BF16)

    @pl.when(yh == 0)
    def _():
        gather_k.across().start()

    for dx in offsets:
        gather_k.along(dx).start()
    gather_k.twin_near(0).start()
    o_across.wait_recv()
    for i in range(len(near)):
        o_side(1, i).start()
    o_twin(1, 0).start()

    fold = 0.125 * LOG2E
    for i in range(PAIRS):
        u = acc[:, 128 * i : 128 * (i + 1)]
        turned = (u * cos + swapped(u) * signed) * fold
        q_all[2 * i] = jnp.where(low, turned, 0.0).astype(BF16)
        q_all[2 * i + 1] = jnp.where(low, pltpu.roll(turned, HEAD_DIM, 1), 0.0).astype(BF16)

    q_pos = lax.broadcasted_iota(jnp.int32, (ROWS, 128), 0) + r * ROWS
    k_off = lax.broadcasted_iota(jnp.int32, (ROWS, 128), 1)

    def make_bias(b):
        for part in range(ROWS // 128):
            keys = kv_all[b, ROWS + part : ROWS + part + 1, :].astype(F32)
            seen = (docs_col[...] == keys) & (k_off + (b * ROWS + part * 128) <= q_pos)
            bias[b, :, part * 128 : (part + 1) * 128] = jnp.where(seen, 0.0, NEG)
        block = kv_all[b, 0:ROWS, :]
        v_all[b] = jnp.where(low, 1.0, block.astype(F32)).astype(BF16)

    def attend(b, h, count, fresh=False):
        heads = pl.ds(h, count)
        scores = lax.dot_general(
            q_all[heads].reshape(count * ROWS, 128),
            kv_all[b, 0:ROWS, :],
            (((1,), (1,)), ((), ())),
            preferred_element_type=F32,
        )
        weights = jnp.exp2(scores.reshape(count, ROWS, ROWS) + bias[b][None]).astype(BF16)
        added = jnp.dot(
            weights.reshape(count * ROWS, ROWS), v_all[b], preferred_element_type=F32
        ).reshape(count, ROWS, 128)
        if fresh:
            o_acc[heads] = added
        else:
            o_acc[heads] += added

    STACK = PAIRS

    make_bias(r)

    attend(r, 0, STACK, True)
    attend(r, STACK, STACK, True)

    for dx in offsets:
        gather_k.along(dx).wait_recv()
        gather_k.twin_near(dx).start()

    @pl.when(yh == 1)
    def _():
        gather_k.across().wait_recv()
        for dx in offsets:
            gather_k.along_other(dx).start()
        gather_k.twin_other(0).start()

    for dx in range(NX):
        gather_k.twin_near(dx).wait_recv()

    def near_block(b, _):
        make_bias(b)
        attend(b, 0, STACK)
        attend(b, STACK, STACK)
        return 0

    lax.fori_loop(yh * HALF, r, near_block, 0)

    @pl.when(yh == 1)
    def _():
        for dx in offsets:
            gather_k.along_other(dx).wait_recv()
            gather_k.twin_other(dx).start()

    o_take_far(0)
    o_take_sides(1)

    far_from = jnp.maximum(r - REACH, 0)
    far_to = jnp.where(yh == 1, HALF, far_from)

    @pl.when(yh == 1)
    def _():
        for dx in range(NX):
            gather_k.twin_other(dx).wait_recv()

        def far_bias(b, _):
            make_bias(b)
            return 0

        lax.fori_loop(far_from, HALF, far_bias, 0)

    def sink_of(h):
        return jnp.exp(jnp.full((1, 128), sinks[h], F32))

    def ctx_copy(i, dt):
        ref = ctx.at[t, i]
        return remote(
            ref, ref, ctx_send.at[i, dt], ctx_recv.at[i, dt], {"tensor": lax.rem(t + dt, NT)}
        )

    ends = NT == 4

    def direct(dt):
        if not ends:
            return t >= 0
        return jnp.abs(lax.rem(t + dt, NT) - t) < 3

    def ctx_pass(i, dt):
        ref = ctx.at[lax.rem(t + 2, NT), i]
        return remote(
            ref,
            ref,
            pass_send.at[i],
            ctx_recv.at[i, dt],
            {"tensor": lax.rem(t + dt + 2, NT)},
        )

    def finish_stack(k, _):
        def far_block(b, _):
            attend(b, STACK * k, STACK)
            return 0

        lax.fori_loop(far_from, far_to, far_block, 0)
        for n in range(STACK // 2):
            i = k * (STACK // 2) + n
            even = o_acc[2 * i]
            odd = o_acc[2 * i + 1]
            even = pltpu.roll(even, HEAD_DIM, 1) / (even + sink_of(2 * i))
            odd = odd / (pltpu.roll(odd, HEAD_DIM, 1) + sink_of(2 * i + 1))
            ctx[t, i] = jnp.where(low, even, odd).astype(BF16)
            for dt in range(1, NT):

                @pl.when(direct(dt))
                def _(i=i, dt=dt):
                    ctx_copy(i, dt).start()

        return 0

    lax.fori_loop(0, 2, finish_stack, 0)

    def project(tt):
        total = None
        for i in range(0, PAIRS, 2):
            role = tt * (R // NT) + i
            rows = jnp.concatenate([wo_all[role], wo_all[role + 1]], axis=1)
            heads = jnp.concatenate([ctx[tt, i], ctx[tt, i + 1]], axis=1)
            part = lax.dot_general(
                rows, heads, (((1,), (1,)), ((), ())), preferred_element_type=F32
            )
            total = part if total is None else total + part
        return total

    if ends:
        for where, dt in ((1, 1), (2, 3)):

            @pl.when(t == where)
            def _(dt=dt):
                for i in range(PAIRS):
                    ctx_copy(i, 2).wait_recv()
                    ctx_pass(i, dt).start()

    o_take_far(1)
    for dy in range(2):
        for dx in range(NX):
            o_twin(dy, dx).wait_recv()
    out_acc[...] = project(t)
    order = (1, 3, 2) if ends else tuple(range(1, NT))
    for dt in order:
        if ends and dt == 2:

            @pl.when((t == 0) | (t == 3))
            def _():
                for i in range(PAIRS):
                    ctx_copy(i, dt).wait_recv()
        else:
            for i in range(PAIRS):
                ctx_copy(i, dt).wait_recv()
        out_acc[...] += project(lax.rem(t + NT - dt, NT))
    out[...] = out_acc[...].astype(BF16)

    for copy in [w_across, o_across] + w_far + w_beyond:
        copy.wait_send()
    for dy in range(2):
        for i in range(len(near)):
            o_side(dy, i).wait_send()
            if far:
                o_on(dy, i).wait_send()
        for dx in range(NX):
            o_twin(dy, dx).wait_send()

    @pl.when(yh == 0)
    def _():
        gather_k.across().wait_send()

    for dx in offsets:
        gather_k.along(dx).wait_send()
    for dx in range(NX):
        gather_k.twin_near(dx).wait_send()

    @pl.when(yh == 1)
    def _():
        for dx in offsets:
            gather_k.along_other(dx).wait_send()
        for dx in range(NX):
            gather_k.twin_other(dx).wait_send()

    for j in travels:
        for s in range(H):
            for d in range(2):
                if s < H - 1 or d == last(j):
                    ring(d, s, j).wait_send()
    for s in range(H + 1):
        for d in both(s):
            for copy in sides(d, s) + [twin_plane(d, s)]:
                copy.wait_send()
    for i in range(PAIRS):
        for dt in range(1, NT):

            @pl.when(direct(dt))
            def _(i=i, dt=dt):
                ctx_copy(i, dt).wait_send()

    if ends:

        @pl.when((t == 1) | (t == 2))
        def _():
            for i in range(PAIRS):
                ctx_pass(i, 1).wait_send()


def rotation_tables(rows, roles):
    half = HEAD_DIM // 2
    freq = np.exp(-math.log(150000.0) * np.arange(half) / half)
    freq = np.tile(freq, 128 // half)[None, :]
    near = np.arange(rows)[:, None] * freq
    far = (np.arange(roles) * rows)[:, None] * freq
    return [a.astype(np.float32) for a in (np.cos(near), np.sin(near), np.cos(far), np.sin(far))]


def on_device(sizes, tokens, gain, q_weight, kv_weight, out_weight, sinks, segments):
    NG, NT, R = sizes
    feature = tokens[0].T
    width, rows = feature.shape
    NX = R // 4
    heads = q_weight.shape[1] // HEAD_DIM
    columns = q_weight.shape[1] + kv_weight.shape[1]
    features_out = out_weight.shape[1]
    tables = [jnp.asarray(a) for a in rotation_tables(rows, R)]
    H = NG // 2
    dims = (NG, NT, R, NX, rows, width)
    vmem = pl.BlockSpec(memory_space=pltpu.VMEM)
    anywhere = pl.BlockSpec(memory_space=pl.ANY)
    dma = pltpu.SemaphoreType.DMA
    out = pl.pallas_call(
        functools.partial(kernel, dims),
        out_shape=jax.ShapeDtypeStruct((features_out, rows), BF16),
        in_specs=[anywhere, vmem, vmem, vmem, anywhere, vmem]
        + [pl.BlockSpec(memory_space=pltpu.SMEM)]
        + [vmem] * 4,
        out_specs=vmem,
        scratch_shapes=[
            pltpu.VMEM((width, rows), BF16),
            pltpu.VMEM((width, rows), BF16),
            pltpu.VMEM((NG, rows, R * 16), BF16),
            pltpu.VMEM((16, columns), BF16),
            pltpu.VMEM((NG, R, 16, columns), BF16),
            pltpu.VMEM((rows, columns), F32),
            pltpu.VMEM((heads, rows, 128), BF16),
            pltpu.VMEM((R, rows + 16, 128), BF16),
            pltpu.VMEM((R, rows, 128), BF16),
            pltpu.VMEM((rows, 128), F32),
            pltpu.VMEM((R, rows, rows), F32),
            pltpu.VMEM((heads, rows, 128), F32),
            pltpu.VMEM((R, features_out, 128), BF16),
            pltpu.VMEM((NT, heads // 2, rows, 128), BF16),
            pltpu.VMEM((features_out, rows), F32),
            dma((2,)),
            dma((3, 9 + 2 * NX)),
            dma((3, 9 + 2 * NX)),
            dma((2, H, R // 2)),
            dma((2, H, R // 2)),
            dma((2, H + 1, 4)),
            dma((2, H + 1, 4)),
            dma((2, H + 1)),
            dma((2, H + 1)),
            dma((heads // 2, NT)),
            dma((heads // 2, NT)),
            dma((heads // 2,)),
        ],
        compiler_params=pltpu.CompilerParams(collective_id=0, has_side_effects=True),
        name="layer",
    )(
        feature,
        gain,
        q_weight,
        kv_weight,
        out_weight.T,
        segments,
        sinks,
        *tables,
    )
    return out.T[None]


def solution(mesh):
    placed = (
        P("group", "role", None),
        P(),
        P(("group", "role"), "tensor"),
        P(("group", "role"), "tensor"),
        P("role", "tensor"),
        P("tensor"),
        P("group", "role"),
    )
    sizes = (mesh.shape["group"], mesh.shape["tensor"], mesh.shape["role"])
    return jax.shard_map(
        functools.partial(on_device, sizes),
        mesh=mesh,
        in_specs=placed,
        out_specs=P("group", "role", "tensor"),
        check_vma=False,
    )
```

```python
import functools
import math

import jax
import jax.numpy as jnp
import numpy as np
from jax import lax
from jax.experimental import pallas as pl
from jax.experimental.pallas import tpu as pltpu
from jax.sharding import PartitionSpec as P

HEAD_DIM = 64
REACH = 9
NEG = -1e30
LOG2E = 1.4426950408889634
F32 = jnp.float32
BF16 = jnp.bfloat16


def kernel(
    dims,
    tokens_hbm,
    gain,
    wq_in,
    wkv_in,
    wo_hbm,
    docs_in,
    sinks,
    near_cos,
    near_sin,
    far_cos,
    far_sin,
    out,
    tokens,
    normed,
    spread,
    w_own,
    w_all,
    acc,
    q_all,
    kv_all,
    v_all,
    docs_col,
    bias,
    o_acc,
    wo_all,
    ctx,
    around,
    out_acc,
    load_sem,
    plane_send,
    plane_recv,
    ring_send,
    ring_recv,
    side_send,
    side_recv,
    twin_send,
    twin_recv,
    ctx_send,
    ctx_recv,
    pass_send,
    around_send,
    around_recv,
):
    NG, NT, R, NX, ROWS, D = dims
    HALF = R // 2
    H = NG // 2
    PAIRS = q_all.shape[0] // 2
    WIDE = q_all.shape[0] * HEAD_DIM
    g = lax.axis_index("group")
    t = lax.axis_index("tensor")
    r = lax.axis_index("role")
    c = lax.rem(r, 2)
    x = lax.rem(r // 2, NX)
    yh = r // HALF

    def role_of(y_, x_, c_):
        return y_ * HALF + x_ * 2 + c_

    def x_at(dx):
        return lax.rem(x + dx, NX)

    twin = {"role": role_of(yh, x, 1 - c)}
    across = {"role": role_of(1 - yh, x, c)}

    beyond = {"role": role_of(1 - yh, x_at(NX // 2), c)}

    def x_to(dx):
        return {"role": role_of(yh, x_at(dx), c)}

    def along_ring(d, hop):
        return {"group": lax.rem(g + hop, NG) if d == 0 else lax.rem(g + NG - hop, NG)}


    def remote(src, dst, send, recv, where):
        return pltpu.make_async_remote_copy(
            src_ref=src,
            dst_ref=dst,
            send_sem=send,
            recv_sem=recv,
            device_id=where,
            device_id_type=pl.DeviceIdType.MESH,
        )

    load_tokens = pltpu.make_async_copy(tokens_hbm, tokens, load_sem.at[0])
    load_tokens.start()
    load_wo = pltpu.make_async_copy(wo_hbm, wo_all.at[r], load_sem.at[1])
    load_wo.start()
    w_own[0:15, 0:WIDE] = wq_in[...]
    w_own[0:15, WIDE : WIDE + 128] = wkv_in[...]
    w_own[15:16, :] = jnp.zeros((1, WIDE + 128), BF16)

    greeted = [twin, across] + [along_ring(d, hop) for d in range(2) for hop in (1, 2)]
    greeted += [x_to(dx) for dx in range(1, NX)]
    if NX > 2:
        greeted += [beyond]
    ends = NT == 4
    middle = (t == 1) | (t == 2)
    if ends:
        other = role_of(1 - yh, x, c)
        greeted += [
            {"tensor": jnp.where(middle, 0, 1), "role": other},
            {"tensor": jnp.where(middle, 3, 2), "role": other},
        ]
    greeted += [{"tensor": lax.rem(t + dt, NT)} for dt in range(1, NT)]
    barrier = pltpu.get_barrier_semaphore()
    for where in greeted:
        pl.semaphore_signal(
            barrier, inc=1, device_id=where, device_id_type=pl.DeviceIdType.MESH
        )
    pl.semaphore_wait(barrier, len(greeted))

    class Gather:
        def __init__(self, which, own, slot):
            self.send = plane_send.at[which]
            self.recv = plane_recv.at[which]
            self.own = own
            self.slot = slot

        def copy(self, index, role, where, src=None):
            dst = self.slot(role)
            return remote(
                dst if src is None else src, dst, self.send.at[index], self.recv.at[index], where
            )

        def across(self):
            return self.copy(0, r, across, self.own)

        def along(self, dx):
            return self.copy(dx, r, x_to(dx), self.own)

        def along_other(self, dx):
            return self.copy(NX - 1 + dx, role_of(1 - yh, x, c), x_to(dx))

        def twin_near(self, dx):
            if dx == 0:
                return self.copy(2 * NX, r, twin, self.own)
            return self.copy(2 * NX + dx, role_of(yh, lax.rem(x + NX - dx, NX), c), twin)

        def twin_other(self, dx):
            return self.copy(3 * NX + dx, role_of(1 - yh, lax.rem(x + NX - dx, NX), c), twin)

    gather_k = Gather(2, kv_all.at[r], lambda role: kv_all.at[role])
    offsets = range(1, NX)

    far = [2] if NX > 2 else []
    near = [1, NX - 1] if NX > 2 else [1]
    upper = (wo_all.shape[1] // 2) // 16 * 16

    def own_block(slot):
        return w_all.at[g, c * HALF + slot]

    def w_copy(index, slot, where):
        return remote(
            w_own, own_block(slot), plane_send.at[0, index], plane_recv.at[0, index], where
        )

    w_across = w_copy(0, NX, across)
    w_far = [w_copy(1, dx, x_to(dx)) for dx in far]
    w_beyond = [w_copy(2, NX + dx, beyond) for dx in far]
    travels = {0: 0.0, NX: 6.0}
    for dx in far:
        travels.update({dx: 3.0, NX + dx: 7.5})

    def plane(d, s):
        return lax.rem(g - s + NG, NG) if d == 0 else lax.rem(g + s, NG)

    def ring(d, s, j):
        hop = 2 if s % 2 == 0 else 1
        dst = w_all.at[plane(d, s - hop), c * HALF + j]
        return remote(
            w_own if s == hop and j == 0 else dst,
            dst,
            ring_send.at[d, s - 1, j],
            ring_recv.at[d, s - 1, j],
            along_ring(d, hop),
        )

    def side(d, s, j, i):
        slot = c * HALF + j
        index = (d, s, 2 * (j // NX) + i)
        return remote(
            w_own if s == 0 and j == 0 else w_all.at[plane(d, s), slot],
            w_all.at[plane(d, s), slot + near[i]],
            side_send.at[index],
            side_recv.at[index],
            x_to(near[i]),
        )

    def sides(d, s):
        return [side(d, s, j, i) for j in (0, NX) for i in range(len(near))]

    def both(s):
        return range(2 if 0 < s < H else 1)

    def o_copy(index, role, where, rows=None):
        ref = wo_all.at[role] if rows is None else wo_all.at[role, rows]
        return remote(ref, ref, plane_send.at[1, index], plane_recv.at[1, index], where)

    def behind(y_, dx):
        return role_of(y_, lax.rem(x + NX - dx, NX), c)

    def halves():
        return (pl.ds(0, upper), pl.ds(upper, wo_all.shape[1] - upper))

    o_across = o_copy(0, r, across)

    def o_side(dy, i):
        return o_copy(1 + 4 * dy + i, behind(yh if dy == 0 else 1 - yh, 0), x_to(near[i]))

    def o_on(dy, i):
        role = behind(yh if dy == 0 else 1 - yh, near[i])
        return o_copy(3 + 4 * dy + i, role, x_to(near[i]), halves()[i])

    def o_twin(dy, dx):
        return o_copy(9 + dy * NX + dx, behind(yh if dy == 0 else 1 - yh, dx), twin)

    def o_take_sides(dy):
        for i in range(len(near)):
            o_side(dy, i).wait_recv()
            if far:
                o_on(dy, i).start()
            o_twin(dy, near[i]).start()

    def o_take_far(dy):
        for dx in far:
            for i in range(2):
                o_on(dy, i).wait_recv()
            o_twin(dy, dx).start()

    def twin_plane(d, s):
        ref = w_all.at[plane(d, s), pl.ds(c * HALF, HALF)]
        return remote(ref, ref, twin_send.at[d, s], twin_recv.at[d, s], twin)

    def last(j):
        return j // NX

    def add_plane(p):
        acc[...] += jnp.dot(
            spread[p],
            w_all[p].reshape(R * 16, acc.shape[1]),
            preferred_element_type=F32,
        )

    def ways(s, j):
        return (last(j),) if s == H else (0, 1)

    def onward(s, j):
        return [s + hop for hop in (1, 2) if s % 2 == 0 and s + hop <= H]

    def take(s, j):
        if s == 0 and j == NX:
            w_across.wait_recv()
        elif s == 0 and j > NX:
            w_beyond[0].wait_recv()
        elif s == 0 and j > 0:
            w_far[0].wait_recv()
        for d in range(2):
            if s > 0 and d in ways(s, j):
                ring(d, s, j).wait_recv()
            for to in onward(s, j)[::-1]:
                if d in ways(to, j):
                    ring(d, to, j).start()
        if j % NX == 0:
            for d in both(s):
                for i in range(len(near)):
                    side(d, s, j, i).start()

    def share(s):
        for d in both(s):
            for copy in sides(d, s):
                copy.wait_recv()
            twin_plane(d, s).start()

    def add_planes(s):
        for d in both(s):
            twin_plane(d, s).wait_recv()
            add_plane(plane(d, s))

    w_across.start()
    for copy in w_beyond + w_far:
        copy.start()
    take(0, 0)
    w_all[g, c * HALF] = w_own[...]
    load_wo.wait()
    o_across.start()
    for i in range(len(near)):
        o_side(0, i).start()
    o_twin(0, 0).start()

    load_tokens.wait()

    def add_squares(i, total):
        wide = tokens[pl.ds(pl.multiple_of(i * 160, 32), 160), :].astype(F32)
        return total + jnp.sum((wide * wide).reshape(20, 8, ROWS), axis=0)

    squares = lax.fori_loop(0, D // 160, add_squares, jnp.zeros((8, ROWS), F32))
    scale = lax.rsqrt(jnp.sum(squares, axis=0, keepdims=True) * (1.0 / D) + 1e-05)

    def norm_rows(start, count):
        row = jnp.broadcast_to(gain[pl.ds(start, count)][None], (128, count))
        column = jnp.transpose(row)
        wide = tokens[pl.ds(start, count), :].astype(F32)
        normed[pl.ds(start, count), :] = (
            wide * scale * jnp.concatenate([column] * (ROWS // 128), axis=1)
        ).astype(BF16)

    def norm_full(i, _):
        norm_rows(pl.multiple_of(i * 128, 128), 128)
        return 0

    lax.fori_loop(0, D // 128, norm_full, 0)
    if D % 128:
        norm_rows(D // 128 * 128, D % 128)
    lane = lax.broadcasted_iota(jnp.int32, (15 * R, R * 16), 1)
    slot_of = lane // 16
    within = lax.rem(lane, 16)
    rel = lax.rem(slot_of, HALF)
    slot_role = role_of(
        lax.rem(yh + rel // NX, 2), lax.rem(x + NX - lax.rem(rel, NX), NX), slot_of // HALF
    )
    feature = jnp.where(within < 15, slot_role * 15 + within, -1)
    hit = lax.broadcasted_iota(jnp.int32, (15 * R, R * 16), 0) == feature
    pick = jnp.where(hit, 1.0, 0.0).astype(BF16)

    def spread_plane(p, _):
        part = normed[pl.ds(pl.multiple_of(p * (15 * R), 8), 15 * R), :]
        spread[p] = lax.dot_general(
            part, pick, (((0,), (0,)), ((), ())), preferred_element_type=F32
        ).astype(BF16)
        return 0

    def spread_planes(part):
        lax.fori_loop(part * (NG // 2), (part + 1) * (NG // 2), spread_plane, 0)

    acc[...] = jnp.zeros_like(acc)
    docs = docs_in[...].astype(F32)
    for part in range(ROWS // 128):
        row = jnp.broadcast_to(docs[:, 128 * part : 128 * (part + 1)], (128, 128))
        docs_col[128 * part : 128 * (part + 1), :] = jnp.transpose(row)
    STEP, SKIP = 3.4, 4.4

    def due(s, j):
        return travels[j] + (s // 2) * SKIP + (s % 2) * STEP

    tasks = []
    for s in range(H + 1):
        for j in travels:
            if s > 0 or j > 0:
                tasks.append((due(s, j), functools.partial(take, s, j)))
        there = max(max(due(s, j) for j in travels), max(due(s, 0), due(s, NX)) + STEP)
        tasks.append((there, functools.partial(share, s)))
        tasks.append((there + 4.0 if s <= H // 3 else 90.0 + s, functools.partial(add_planes, s)))
    tasks.append((14.0, functools.partial(o_take_sides, 0)))
    tasks.append((3.8, functools.partial(spread_planes, 0)))
    tasks.append((8.2, functools.partial(spread_planes, 1)))
    for _, task in sorted(tasks, key=lambda one: one[0]):
        task()
    cos_far = far_cos[pl.ds(r, 1), :]
    sin_far = far_sin[pl.ds(r, 1), :]
    cos = near_cos[...] * cos_far - near_sin[...] * sin_far
    sin = near_sin[...] * cos_far + near_cos[...] * sin_far
    lanes = lax.broadcasted_iota(jnp.int32, (ROWS, 128), 1)
    first_half = lax.rem(lanes, HEAD_DIM) < HEAD_DIM // 2
    low = lanes < HEAD_DIM
    signed = jnp.where(first_half, -sin, sin)

    def swapped(u):
        return jnp.where(
            first_half, pltpu.roll(u, 128 - HEAD_DIM // 2, 1), pltpu.roll(u, HEAD_DIM // 2, 1)
        )

    pair = acc[:, WIDE : WIDE + 128]
    turned = pair * jnp.where(low, cos, 1.0) + swapped(pair) * jnp.where(low, signed, 0.0)
    kv_all[r, 0:ROWS] = turned.astype(BF16)
    doc_rows = jnp.zeros((16, 128), F32)
    line = lax.broadcasted_iota(jnp.int32, (16, 128), 0)
    for part in range(ROWS // 128):
        doc_rows = jnp.where(line == part, docs[:, 128 * part : 128 * (part + 1)], doc_rows)
    kv_all[r, ROWS : ROWS + 16] = doc_rows.astype(BF16)

    @pl.when(yh == 0)
    def _():
        gather_k.across().start()

    for dx in offsets:
        gather_k.along(dx).start()
    gather_k.twin_near(0).start()
    o_across.wait_recv()
    for i in range(len(near)):
        o_side(1, i).start()
    o_twin(1, 0).start()

    fold = 0.125 * LOG2E
    for i in range(PAIRS):
        u = acc[:, 128 * i : 128 * (i + 1)]
        turned = (u * cos + swapped(u) * signed) * fold
        q_all[2 * i] = jnp.where(low, turned, 0.0).astype(BF16)
        q_all[2 * i + 1] = jnp.where(low, pltpu.roll(turned, HEAD_DIM, 1), 0.0).astype(BF16)

    q_pos = lax.broadcasted_iota(jnp.int32, (ROWS, 128), 0) + r * ROWS
    k_off = lax.broadcasted_iota(jnp.int32, (ROWS, 128), 1)

    def make_bias(b):
        for part in range(ROWS // 128):
            keys = kv_all[b, ROWS + part : ROWS + part + 1, :].astype(F32)
            seen = (docs_col[...] == keys) & (k_off + (b * ROWS + part * 128) <= q_pos)
            bias[b, :, part * 128 : (part + 1) * 128] = jnp.where(seen, 0.0, NEG)
        block = kv_all[b, 0:ROWS, :]
        v_all[b] = jnp.where(low, 1.0, block.astype(F32)).astype(BF16)

    def attend(b, h, count, fresh=False):
        heads = pl.ds(h, count)
        scores = lax.dot_general(
            q_all[heads].reshape(count * ROWS, 128),
            kv_all[b, 0:ROWS, :],
            (((1,), (1,)), ((), ())),
            preferred_element_type=F32,
        )
        weights = jnp.exp2(scores.reshape(count, ROWS, ROWS) + bias[b][None]).astype(BF16)
        added = jnp.dot(
            weights.reshape(count * ROWS, ROWS), v_all[b], preferred_element_type=F32
        ).reshape(count, ROWS, 128)
        if fresh:
            o_acc[heads] = added
        else:
            o_acc[heads] += added

    STACK = PAIRS

    make_bias(r)

    attend(r, 0, STACK, True)
    attend(r, STACK, STACK, True)

    for dx in offsets:
        gather_k.along(dx).wait_recv()
        gather_k.twin_near(dx).start()

    @pl.when(yh == 1)
    def _():
        gather_k.across().wait_recv()
        for dx in offsets:
            gather_k.along_other(dx).start()
        gather_k.twin_other(0).start()

    for dx in range(NX):
        gather_k.twin_near(dx).wait_recv()

    def near_block(b, _):
        make_bias(b)
        attend(b, 0, STACK)
        attend(b, STACK, STACK)
        return 0

    lax.fori_loop(yh * HALF, jnp.where(yh == 1, r, 0), near_block, 0)

    @pl.when(yh == 1)
    def _():
        gather_k.twin_other(0).wait_recv()
        near_block(role_of(0, x, c), 0)
        near_block(role_of(0, x, 1 - c), 0)

    @pl.when(yh == 1)
    def _():
        for dx in offsets:
            gather_k.along_other(dx).wait_recv()
            gather_k.twin_other(dx).start()

    o_take_far(0)
    o_take_sides(1)

    far_from = jnp.maximum(r - REACH, 0)
    far_to = jnp.where(yh == 1, HALF, r)

    @pl.when(yh == 1)
    def _():
        for dx in offsets:
            gather_k.twin_other(dx).wait_recv()

    def in_finish(b):
        return (yh == 0) | (b // 2 != x)

    def far_bias(b, _):
        @pl.when(in_finish(b))
        def _():
            make_bias(b)

        return 0

    lax.fori_loop(far_from, far_to, far_bias, 0)

    def sink_of(h):
        return jnp.exp(jnp.full((1, 128), sinks[h], F32))

    def ctx_copy(i, dt):
        ref = ctx.at[t, i]
        return remote(
            ref, ref, ctx_send.at[i, dt], ctx_recv.at[i, dt], {"tensor": lax.rem(t + dt, NT)}
        )

    def direct(dt):
        if not ends:
            return t >= 0
        apart = jnp.abs(lax.rem(t + dt, NT) - t)
        return (apart == 1) | ((apart == 2) & jnp.logical_not(middle))

    to_end = jnp.where(t == 1, 0, 3)
    turning = STACK // 2
    rounds = x < NX // 2

    def ctx_pass(i, kind):
        source = 3 - t if kind == 0 else jnp.where(t == 1, 3, 0)
        ref = ctx.at[source, i]
        back = lax.rem(to_end + NT - source, NT)
        return remote(
            ref, ref, pass_send.at[kind, i], ctx_recv.at[i, back], {"tensor": to_end}
        )

    def around_out(i):
        return remote(
            ctx.at[t, i],
            around.at[i],
            around_send.at[0, i],
            around_recv.at[i],
            {"tensor": jnp.where(t == 0, 2, 1), "role": role_of(0, x, c)},
        )

    def around_on(i):
        source = jnp.where(t == 2, 0, 3)
        return remote(
            around.at[i],
            ctx.at[source, i],
            around_send.at[1, i],
            ctx_recv.at[i, lax.rem(3 - source + NT - source, NT)],
            {"tensor": 3 - source, "role": role_of(1, x, c)},
        )

    def finish_stack(k, _):
        def far_block(b, _):
            @pl.when(in_finish(b))
            def _():
                attend(b, STACK * k, STACK)

            return 0

        lax.fori_loop(far_from, far_to, far_block, 0)
        for n in range(STACK // 2):
            i = k * (STACK // 2) + n
            even = o_acc[2 * i]
            odd = o_acc[2 * i + 1]
            even = pltpu.roll(even, HEAD_DIM, 1) / (even + sink_of(2 * i))
            odd = odd / (pltpu.roll(odd, HEAD_DIM, 1) + sink_of(2 * i + 1))
            ctx[t, i] = jnp.where(low, even, odd).astype(BF16)
            if ends:

                @pl.when((yh == 1) & rounds & jnp.logical_not(middle) & (k == 0))
                def _(i=i):
                    around_out(i).start()

            for dt in (2, 1, 3)[: NT - 1] if ends else range(1, NT):

                @pl.when(direct(dt))
                def _(i=i, dt=dt):
                    ctx_copy(i, dt).start()

        return 0

    lax.fori_loop(0, 2, finish_stack, 0)

    def project(tt):
        total = None
        for i in range(0, PAIRS, 2):
            role = tt * (R // NT) + i
            rows = jnp.concatenate([wo_all[role], wo_all[role + 1]], axis=1)
            heads = jnp.concatenate([ctx[tt, i], ctx[tt, i + 1]], axis=1)
            part = lax.dot_general(
                rows, heads, (((1,), (1,)), ((), ())), preferred_element_type=F32
            )
            total = part if total is None else total + part
        return total

    if ends:

        @pl.when(middle)
        def _():
            def relay(i):
                ctx_copy(i, 2).wait_recv()
                ctx_pass(i, 1).start()

            for i in range(PAIRS):
                ctx_copy(i, jnp.where(t == 1, 3, 1)).wait_recv()
                ctx_pass(i, 0).start()
                if i >= turning:
                    relay(i)
                else:
                    pl.when((yh == 0) | jnp.logical_not(rounds))(functools.partial(relay, i))

            @pl.when((yh == 0) & rounds)
            def _():
                for i in range(turning):
                    around_out(i).wait_recv()
                    around_on(i).start()

    o_take_far(1)
    for dy in range(2):
        for dx in range(NX):
            o_twin(dy, dx).wait_recv()
    out_acc[...] = project(t)
    for k in range(1, NT):
        source = lax.rem(t + k, NT)
        if ends:
            order = ((1, 2, 3), (0, 2, 3), (1, 3, 0), (2, 1, 0))
            source = order[3][k - 1]
            for where in range(3):
                source = jnp.where(t == where, order[where][k - 1], source)
        dt = lax.rem(t + NT - source, NT)
        for i in range(PAIRS):
            waited = (t < 0) | (t > NT)
            if ends:
                passed = dt == 2
                if i < turning:
                    passed = passed & ((yh == 0) | jnp.logical_not(rounds))
                waited = middle & ((source == 1) | (source == 2) | passed)

            @pl.when(jnp.logical_not(waited))
            def _(i=i, dt=dt):
                ctx_copy(i, dt).wait_recv()

        out_acc[...] += project(source)
    out[...] = out_acc[...].astype(BF16)

    for copy in [w_across, o_across] + w_far + w_beyond:
        copy.wait_send()
    for dy in range(2):
        for i in range(len(near)):
            o_side(dy, i).wait_send()
            if far:
                o_on(dy, i).wait_send()
        for dx in range(NX):
            o_twin(dy, dx).wait_send()

    @pl.when(yh == 0)
    def _():
        gather_k.across().wait_send()

    for dx in offsets:
        gather_k.along(dx).wait_send()
    for dx in range(NX):
        gather_k.twin_near(dx).wait_send()

    @pl.when(yh == 1)
    def _():
        for dx in offsets:
            gather_k.along_other(dx).wait_send()
        for dx in range(NX):
            gather_k.twin_other(dx).wait_send()

    for j in travels:
        for s in range(1, H + 1):
            for d in ways(s, j):
                ring(d, s, j).wait_send()
    for s in range(H + 1):
        for d in both(s):
            for copy in sides(d, s) + [twin_plane(d, s)]:
                copy.wait_send()
    for i in range(PAIRS):
        for dt in range(1, NT):

            @pl.when(direct(dt))
            def _(i=i, dt=dt):
                ctx_copy(i, dt).wait_send()

    if ends:

        @pl.when(middle)
        def _():
            for i in range(PAIRS):
                ctx_pass(i, 0).wait_send()
                if i >= turning:
                    ctx_pass(i, 1).wait_send()

            @pl.when((yh == 0) | jnp.logical_not(rounds))
            def _():
                for i in range(turning):
                    ctx_pass(i, 1).wait_send()

            @pl.when((yh == 0) & rounds)
            def _():
                for i in range(turning):
                    around_on(i).wait_send()

        @pl.when((yh == 1) & rounds & jnp.logical_not(middle))
        def _():
            for i in range(turning):
                around_out(i).wait_send()


def rotation_tables(rows, roles):
    half = HEAD_DIM // 2
    freq = np.exp(-math.log(150000.0) * np.arange(half) / half)
    freq = np.tile(freq, 128 // half)[None, :]
    near = np.arange(rows)[:, None] * freq
    far = (np.arange(roles) * rows)[:, None] * freq
    return [a.astype(np.float32) for a in (np.cos(near), np.sin(near), np.cos(far), np.sin(far))]


def on_device(sizes, tokens, gain, q_weight, kv_weight, out_weight, sinks, segments):
    NG, NT, R = sizes
    feature = tokens[0].T
    width, rows = feature.shape
    NX = R // 4
    heads = q_weight.shape[1] // HEAD_DIM
    columns = q_weight.shape[1] + kv_weight.shape[1]
    features_out = out_weight.shape[1]
    tables = [jnp.asarray(a) for a in rotation_tables(rows, R)]
    H = NG // 2
    dims = (NG, NT, R, NX, rows, width)
    vmem = pl.BlockSpec(memory_space=pltpu.VMEM)
    anywhere = pl.BlockSpec(memory_space=pl.ANY)
    dma = pltpu.SemaphoreType.DMA
    out = pl.pallas_call(
        functools.partial(kernel, dims),
        out_shape=jax.ShapeDtypeStruct((features_out, rows), BF16),
        in_specs=[anywhere, vmem, vmem, vmem, anywhere, vmem]
        + [pl.BlockSpec(memory_space=pltpu.SMEM)]
        + [vmem] * 4,
        out_specs=vmem,
        scratch_shapes=[
            pltpu.VMEM((width, rows), BF16),
            pltpu.VMEM((width, rows), BF16),
            pltpu.VMEM((NG, rows, R * 16), BF16),
            pltpu.VMEM((16, columns), BF16),
            pltpu.VMEM((NG, R, 16, columns), BF16),
            pltpu.VMEM((rows, columns), F32),
            pltpu.VMEM((heads, rows, 128), BF16),
            pltpu.VMEM((R, rows + 16, 128), BF16),
            pltpu.VMEM((R, rows, 128), BF16),
            pltpu.VMEM((rows, 128), F32),
            pltpu.VMEM((R, rows, rows), F32),
            pltpu.VMEM((heads, rows, 128), F32),
            pltpu.VMEM((R, features_out, 128), BF16),
            pltpu.VMEM((NT, heads // 2, rows, 128), BF16),
            pltpu.VMEM((heads // 2, rows, 128), BF16),
            pltpu.VMEM((features_out, rows), F32),
            dma((2,)),
            dma((3, 9 + 2 * NX)),
            dma((3, 9 + 2 * NX)),
            dma((2, H, R // 2)),
            dma((2, H, R // 2)),
            dma((2, H + 1, 4)),
            dma((2, H + 1, 4)),
            dma((2, H + 1)),
            dma((2, H + 1)),
            dma((heads // 2, NT)),
            dma((heads // 2, NT)),
            dma((2, heads // 2)),
            dma((2, heads // 2)),
            dma((heads // 2,)),
        ],
        compiler_params=pltpu.CompilerParams(collective_id=0, has_side_effects=True),
        name="layer",
    )(
        feature,
        gain,
        q_weight,
        kv_weight,
        out_weight.T,
        segments,
        sinks,
        *tables,
    )
    return out.T[None]


def solution(mesh):
    placed = (
        P("group", "role", None),
        P(),
        P(("group", "role"), "tensor"),
        P(("group", "role"), "tensor"),
        P("role", "tensor"),
        P("tensor"),
        P("group", "role"),
    )
    sizes = (mesh.shape["group"], mesh.shape["tensor"], mesh.shape["role"])
    return jax.shard_map(
        functools.partial(on_device, sizes),
        mesh=mesh,
        in_specs=placed,
        out_specs=P("group", "role", "tensor"),
        check_vma=False,
    )
```

```python
import functools
import math

import jax
import jax.numpy as jnp
import numpy as np
from jax import lax
from jax.experimental import pallas as pl
from jax.experimental.pallas import tpu as pltpu
from jax.sharding import PartitionSpec as P

HEAD_DIM = 64
REACH = 9
NEG = -1e30
LOG2E = 1.4426950408889634
F32 = jnp.float32
BF16 = jnp.bfloat16


def kernel(
    dims,
    tokens_hbm,
    gain,
    wq_in,
    wkv_in,
    wo_hbm,
    docs_in,
    sinks,
    near_cos,
    near_sin,
    far_cos,
    far_sin,
    out,
    tokens,
    normed,
    spread,
    w_own,
    w_all,
    acc,
    q_all,
    kv_all,
    v_all,
    docs_col,
    bias,
    o_acc,
    wo_all,
    ctx,
    around,
    out_acc,
    load_sem,
    plane_send,
    plane_recv,
    ring_send,
    ring_recv,
    side_send,
    side_recv,
    twin_send,
    twin_recv,
    ctx_send,
    ctx_recv,
    pass_send,
    around_send,
    around_recv,
):
    NG, NT, R, NX, ROWS, D = dims
    HALF = R // 2
    H = NG // 2
    PAIRS = q_all.shape[0] // 2
    WIDE = q_all.shape[0] * HEAD_DIM
    g = lax.axis_index("group")
    t = lax.axis_index("tensor")
    r = lax.axis_index("role")
    c = lax.rem(r, 2)
    x = lax.rem(r // 2, NX)
    yh = r // HALF

    def role_of(y_, x_, c_):
        return y_ * HALF + x_ * 2 + c_

    def x_at(dx):
        return lax.rem(x + dx, NX)

    twin = {"role": role_of(yh, x, 1 - c)}
    across = {"role": role_of(1 - yh, x, c)}

    beyond = {"role": role_of(1 - yh, x_at(NX // 2), c)}

    def x_to(dx):
        return {"role": role_of(yh, x_at(dx), c)}

    def along_ring(d, hop):
        return {"group": lax.rem(g + hop, NG) if d == 0 else lax.rem(g + NG - hop, NG)}


    def remote(src, dst, send, recv, where):
        return pltpu.make_async_remote_copy(
            src_ref=src,
            dst_ref=dst,
            send_sem=send,
            recv_sem=recv,
            device_id=where,
            device_id_type=pl.DeviceIdType.MESH,
        )

    load_tokens = pltpu.make_async_copy(tokens_hbm, tokens, load_sem.at[0])
    load_tokens.start()
    load_wo = pltpu.make_async_copy(wo_hbm, wo_all.at[r], load_sem.at[1])
    load_wo.start()
    w_own[0:15, 0:WIDE] = wq_in[...]
    w_own[0:15, WIDE : WIDE + 128] = wkv_in[...]
    w_own[15:16, :] = jnp.zeros((1, WIDE + 128), BF16)

    greeted = [twin, across] + [along_ring(d, hop) for d in range(2) for hop in (1, 2)]
    greeted += [x_to(dx) for dx in range(1, NX)]
    if NX > 2:
        greeted += [beyond]
    ends = NT == 4
    middle = (t == 1) | (t == 2)
    if ends:
        other = role_of(1 - yh, x, c)
        greeted += [
            {"tensor": jnp.where(middle, 0, 1), "role": other},
            {"tensor": jnp.where(middle, 3, 2), "role": other},
        ]
    greeted += [{"tensor": lax.rem(t + dt, NT)} for dt in range(1, NT)]
    barrier = pltpu.get_barrier_semaphore()
    for where in greeted:
        pl.semaphore_signal(
            barrier, inc=1, device_id=where, device_id_type=pl.DeviceIdType.MESH
        )
    pl.semaphore_wait(barrier, len(greeted))

    class Gather:
        def __init__(self, which, own, slot):
            self.send = plane_send.at[which]
            self.recv = plane_recv.at[which]
            self.own = own
            self.slot = slot

        def copy(self, index, role, where, src=None):
            dst = self.slot(role)
            return remote(
                dst if src is None else src, dst, self.send.at[index], self.recv.at[index], where
            )

        def across(self):
            return self.copy(0, r, across, self.own)

        def along(self, dx):
            return self.copy(dx, r, x_to(dx), self.own)

        def along_other(self, dx):
            return self.copy(NX - 1 + dx, role_of(1 - yh, x, c), x_to(dx))

        def twin_near(self, dx):
            if dx == 0:
                return self.copy(2 * NX, r, twin, self.own)
            return self.copy(2 * NX + dx, role_of(yh, lax.rem(x + NX - dx, NX), c), twin)

        def twin_other(self, dx):
            return self.copy(3 * NX + dx, role_of(1 - yh, lax.rem(x + NX - dx, NX), c), twin)

    gather_k = Gather(2, kv_all.at[r], lambda role: kv_all.at[role])
    offsets = range(1, NX)

    far = [2] if NX > 2 else []
    near = [1, NX - 1] if NX > 2 else [1]
    upper = (wo_all.shape[1] // 2) // 16 * 16

    def own_block(slot):
        return w_all.at[g, c * HALF + slot]

    def w_copy(index, slot, where):
        return remote(
            w_own, own_block(slot), plane_send.at[0, index], plane_recv.at[0, index], where
        )

    w_across = w_copy(0, NX, across)
    w_far = [w_copy(1, dx, x_to(dx)) for dx in far]
    w_beyond = [w_copy(2, NX + dx, beyond) for dx in far]
    travels = {0: 0.0, NX: 6.0}
    for dx in far:
        travels.update({dx: 3.0, NX + dx: 7.5})

    def plane(d, s):
        return lax.rem(g - s + NG, NG) if d == 0 else lax.rem(g + s, NG)

    def ring(d, s, j):
        hop = 2 if s % 2 == 0 else 1
        dst = w_all.at[plane(d, s - hop), c * HALF + j]
        return remote(
            w_own if s == hop and j == 0 else dst,
            dst,
            ring_send.at[d, s - 1, j],
            ring_recv.at[d, s - 1, j],
            along_ring(d, hop),
        )

    def side(d, s, j, i):
        slot = c * HALF + j
        index = (d, s, 2 * (j // NX) + i)
        return remote(
            w_own if s == 0 and j == 0 else w_all.at[plane(d, s), slot],
            w_all.at[plane(d, s), slot + near[i]],
            side_send.at[index],
            side_recv.at[index],
            x_to(near[i]),
        )

    def sides(d, s):
        return [side(d, s, j, i) for j in (0, NX) for i in range(len(near))]

    def both(s):
        return range(2 if 0 < s < H else 1)

    def o_copy(index, role, where, rows=None):
        ref = wo_all.at[role] if rows is None else wo_all.at[role, rows]
        return remote(ref, ref, plane_send.at[1, index], plane_recv.at[1, index], where)

    def behind(y_, dx):
        return role_of(y_, lax.rem(x + NX - dx, NX), c)

    def halves():
        return (pl.ds(0, upper), pl.ds(upper, wo_all.shape[1] - upper))

    o_across = o_copy(0, r, across)

    def o_side(dy, i):
        return o_copy(1 + 4 * dy + i, behind(yh if dy == 0 else 1 - yh, 0), x_to(near[i]))

    def o_on(dy, i):
        role = behind(yh if dy == 0 else 1 - yh, near[i])
        return o_copy(3 + 4 * dy + i, role, x_to(near[i]), halves()[i])

    def o_twin(dy, dx):
        return o_copy(9 + dy * NX + dx, behind(yh if dy == 0 else 1 - yh, dx), twin)

    def o_take_sides(dy):
        for i in range(len(near)):
            o_side(dy, i).wait_recv()
            if far:
                o_on(dy, i).start()
            o_twin(dy, near[i]).start()

    def o_take_far(dy):
        for dx in far:
            for i in range(2):
                o_on(dy, i).wait_recv()
            o_twin(dy, dx).start()

    def twin_plane(d, s):
        ref = w_all.at[plane(d, s), pl.ds(c * HALF, HALF)]
        return remote(ref, ref, twin_send.at[d, s], twin_recv.at[d, s], twin)

    def last(j):
        return j // NX

    def add_plane(p):
        acc[...] += jnp.dot(
            spread[p],
            w_all[p].reshape(R * 16, acc.shape[1]),
            preferred_element_type=F32,
        )

    def ways(s, j):
        return (last(j),) if s == H else (0, 1)

    def onward(s, j):
        return [s + hop for hop in (1, 2) if s % 2 == 0 and s + hop <= H]

    def take(s, j):
        if s == 0 and j == NX:
            w_across.wait_recv()
        elif s == 0 and j > NX:
            w_beyond[0].wait_recv()
        elif s == 0 and j > 0:
            w_far[0].wait_recv()
        for d in range(2):
            if s > 0 and d in ways(s, j):
                ring(d, s, j).wait_recv()
            for to in onward(s, j)[::-1]:
                if d in ways(to, j):
                    ring(d, to, j).start()
        if j % NX == 0:
            for d in both(s):
                for i in range(len(near)):
                    side(d, s, j, i).start()

    def share(s):
        for d in both(s):
            for copy in sides(d, s):
                copy.wait_recv()
            twin_plane(d, s).start()

    def add_planes(s):
        for d in both(s):
            twin_plane(d, s).wait_recv()
            add_plane(plane(d, s))

    w_across.start()
    for copy in w_beyond + w_far:
        copy.start()
    take(0, 0)
    w_all[g, c * HALF] = w_own[...]
    load_wo.wait()
    o_across.start()
    for i in range(len(near)):
        o_side(0, i).start()
    o_twin(0, 0).start()

    load_tokens.wait()

    def add_squares(i, total):
        wide = tokens[pl.ds(pl.multiple_of(i * 160, 32), 160), :].astype(F32)
        return total + jnp.sum((wide * wide).reshape(20, 8, ROWS), axis=0)

    squares = lax.fori_loop(0, D // 160, add_squares, jnp.zeros((8, ROWS), F32))
    scale = lax.rsqrt(jnp.sum(squares, axis=0, keepdims=True) * (1.0 / D) + 1e-05)

    def norm_rows(start, count):
        row = jnp.broadcast_to(gain[pl.ds(start, count)][None], (128, count))
        column = jnp.transpose(row)
        wide = tokens[pl.ds(start, count), :].astype(F32)
        normed[pl.ds(start, count), :] = (
            wide * scale * jnp.concatenate([column] * (ROWS // 128), axis=1)
        ).astype(BF16)

    def norm_full(i, _):
        norm_rows(pl.multiple_of(i * 128, 128), 128)
        return 0

    lax.fori_loop(0, D // 128, norm_full, 0)
    if D % 128:
        norm_rows(D // 128 * 128, D % 128)
    lane = lax.broadcasted_iota(jnp.int32, (15 * R, R * 16), 1)
    slot_of = lane // 16
    within = lax.rem(lane, 16)
    rel = lax.rem(slot_of, HALF)
    slot_role = role_of(
        lax.rem(yh + rel // NX, 2), lax.rem(x + NX - lax.rem(rel, NX), NX), slot_of // HALF
    )
    feature = jnp.where(within < 15, slot_role * 15 + within, -1)
    hit = lax.broadcasted_iota(jnp.int32, (15 * R, R * 16), 0) == feature
    pick = jnp.where(hit, 1.0, 0.0).astype(BF16)

    def spread_plane(p, _):
        part = normed[pl.ds(pl.multiple_of(p * (15 * R), 8), 15 * R), :]
        spread[p] = lax.dot_general(
            part, pick, (((0,), (0,)), ((), ())), preferred_element_type=F32
        ).astype(BF16)
        return 0

    def spread_planes(part):
        lax.fori_loop(part * (NG // 2), (part + 1) * (NG // 2), spread_plane, 0)

    acc[...] = jnp.zeros_like(acc)
    docs = docs_in[...].astype(F32)
    for part in range(ROWS // 128):
        row = jnp.broadcast_to(docs[:, 128 * part : 128 * (part + 1)], (128, 128))
        docs_col[128 * part : 128 * (part + 1), :] = jnp.transpose(row)
    STEP, SKIP = 3.4, 4.4

    def due(s, j):
        return travels[j] + (s // 2) * SKIP + (s % 2) * STEP

    tasks = []
    for s in range(H + 1):
        for j in travels:
            if s > 0 or j > 0:
                tasks.append((due(s, j), functools.partial(take, s, j)))
        there = max(max(due(s, j) for j in travels), max(due(s, 0), due(s, NX)) + STEP)
        tasks.append((there, functools.partial(share, s)))
        tasks.append((there + 4.0 if s <= H // 3 else 90.0 + s, functools.partial(add_planes, s)))
    tasks.append((14.0, functools.partial(o_take_sides, 0)))
    tasks.append((3.8, functools.partial(spread_planes, 0)))
    tasks.append((8.2, functools.partial(spread_planes, 1)))
    for _, task in sorted(tasks, key=lambda one: one[0]):
        task()
    cos_far = far_cos[pl.ds(r, 1), :]
    sin_far = far_sin[pl.ds(r, 1), :]
    cos = near_cos[...] * cos_far - near_sin[...] * sin_far
    sin = near_sin[...] * cos_far + near_cos[...] * sin_far
    lanes = lax.broadcasted_iota(jnp.int32, (ROWS, 128), 1)
    first_half = lax.rem(lanes, HEAD_DIM) < HEAD_DIM // 2
    low = lanes < HEAD_DIM
    signed = jnp.where(first_half, -sin, sin)

    def swapped(u):
        return jnp.where(
            first_half, pltpu.roll(u, 128 - HEAD_DIM // 2, 1), pltpu.roll(u, HEAD_DIM // 2, 1)
        )

    pair = acc[:, WIDE : WIDE + 128]
    turned = pair * jnp.where(low, cos, 1.0) + swapped(pair) * jnp.where(low, signed, 0.0)
    kv_all[r, 0:ROWS] = turned.astype(BF16)
    doc_rows = jnp.zeros((16, 128), F32)
    line = lax.broadcasted_iota(jnp.int32, (16, 128), 0)
    for part in range(ROWS // 128):
        doc_rows = jnp.where(line == part, docs[:, 128 * part : 128 * (part + 1)], doc_rows)
    kv_all[r, ROWS : ROWS + 16] = doc_rows.astype(BF16)

    @pl.when(yh == 0)
    def _():
        gather_k.across().start()

    for dx in offsets:

        @pl.when(x + dx < NX)
        def _(dx=dx):
            gather_k.along(dx).start()

    gather_k.twin_near(0).start()
    o_across.wait_recv()
    for i in range(len(near)):
        o_side(1, i).start()
    o_twin(1, 0).start()

    fold = 0.125 * LOG2E
    for i in range(PAIRS):
        u = acc[:, 128 * i : 128 * (i + 1)]
        turned = (u * cos + swapped(u) * signed) * fold
        q_all[2 * i] = jnp.where(low, turned, 0.0).astype(BF16)
        q_all[2 * i + 1] = jnp.where(low, pltpu.roll(turned, HEAD_DIM, 1), 0.0).astype(BF16)

    q_pos = lax.broadcasted_iota(jnp.int32, (ROWS, 128), 0) + r * ROWS
    k_off = lax.broadcasted_iota(jnp.int32, (ROWS, 128), 1)

    def make_bias(b):
        for part in range(ROWS // 128):
            keys = kv_all[b, ROWS + part : ROWS + part + 1, :].astype(F32)
            seen = (docs_col[...] == keys) & (k_off + (b * ROWS + part * 128) <= q_pos)
            bias[b, :, part * 128 : (part + 1) * 128] = jnp.where(seen, 0.0, NEG)
        block = kv_all[b, 0:ROWS, :]
        v_all[b] = jnp.where(low, 1.0, block.astype(F32)).astype(BF16)

    def attend(b, h, count, fresh=False):
        heads = pl.ds(h, count)
        scores = lax.dot_general(
            q_all[heads].reshape(count * ROWS, 128),
            kv_all[b, 0:ROWS, :],
            (((1,), (1,)), ((), ())),
            preferred_element_type=F32,
        )
        weights = jnp.exp2(scores.reshape(count, ROWS, ROWS) + bias[b][None]).astype(BF16)
        added = jnp.dot(
            weights.reshape(count * ROWS, ROWS), v_all[b], preferred_element_type=F32
        ).reshape(count, ROWS, 128)
        if fresh:
            o_acc[heads] = added
        else:
            o_acc[heads] += added

    STACK = PAIRS

    make_bias(r)

    attend(r, 0, STACK, True)
    attend(r, STACK, STACK, True)

    for dx in offsets:

        @pl.when(x >= dx)
        def _(dx=dx):
            gather_k.along(dx).wait_recv()
            gather_k.twin_near(dx).start()


    @pl.when(yh == 1)
    def _():
        gather_k.across().wait_recv()
        for dx in offsets:
            gather_k.along_other(dx).start()
        gather_k.twin_other(0).start()

    for dx in range(NX):

        @pl.when(x >= dx)
        def _(dx=dx):
            gather_k.twin_near(dx).wait_recv()


    def near_block(b, _):
        make_bias(b)
        attend(b, 0, STACK)
        attend(b, STACK, STACK)
        return 0

    lax.fori_loop(yh * HALF, jnp.where(yh == 1, r, 0), near_block, 0)

    @pl.when(yh == 1)
    def _():
        gather_k.twin_other(0).wait_recv()
        near_block(role_of(0, x, c), 0)
        near_block(role_of(0, x, 1 - c), 0)

    @pl.when(yh == 1)
    def _():
        for dx in offsets:
            gather_k.along_other(dx).wait_recv()
            gather_k.twin_other(dx).start()

    early = (yh == 0) & (x < NX // 2)

    def o_take():
        o_take_far(0)
        o_take_sides(1)

    pl.when(jnp.logical_not(early))(o_take)

    far_from = jnp.maximum(r - REACH, 0)
    far_to = jnp.where(yh == 1, HALF, r)

    @pl.when(yh == 1)
    def _():
        for dx in offsets:
            gather_k.twin_other(dx).wait_recv()

    def in_finish(b):
        return (yh == 0) | (b // 2 != x)

    def far_bias(b, _):
        @pl.when(in_finish(b))
        def _():
            make_bias(b)

        return 0

    lax.fori_loop(far_from, far_to, far_bias, 0)

    def sink_of(h):
        return jnp.exp(jnp.full((1, 128), sinks[h], F32))

    def ctx_copy(i, dt):
        ref = ctx.at[t, i]
        return remote(
            ref, ref, ctx_send.at[i, dt], ctx_recv.at[i, dt], {"tensor": lax.rem(t + dt, NT)}
        )

    def direct(dt):
        if not ends:
            return t >= 0
        apart = jnp.abs(lax.rem(t + dt, NT) - t)
        return (apart == 1) | ((apart == 2) & jnp.logical_not(middle))

    to_end = jnp.where(t == 1, 0, 3)
    def rounds(i):
        return x < (NX // 2 if i < STACK // 2 else NX // 4)


    def ctx_pass(i, kind):
        source = 3 - t if kind == 0 else jnp.where(t == 1, 3, 0)
        ref = ctx.at[source, i]
        back = lax.rem(to_end + NT - source, NT)
        return remote(
            ref, ref, pass_send.at[kind, i], ctx_recv.at[i, back], {"tensor": to_end}
        )

    def around_out(i):
        return remote(
            ctx.at[t, i],
            around.at[i],
            around_send.at[0, i],
            around_recv.at[i],
            {"tensor": jnp.where(t == 0, 2, 1), "role": role_of(0, x, c)},
        )

    def around_on(i):
        source = jnp.where(t == 2, 0, 3)
        return remote(
            around.at[i],
            ctx.at[source, i],
            around_send.at[1, i],
            ctx_recv.at[i, lax.rem(3 - source + NT - source, NT)],
            {"tensor": 3 - source, "role": role_of(1, x, c)},
        )

    def finish_stack(k, _):
        def far_block(b, _):
            @pl.when(in_finish(b))
            def _():
                attend(b, STACK * k, STACK)

            return 0

        lax.fori_loop(far_from, far_to, far_block, 0)
        for n in range(STACK // 2):
            i = k * (STACK // 2) + n
            even = o_acc[2 * i]
            odd = o_acc[2 * i + 1]
            even = pltpu.roll(even, HEAD_DIM, 1) / (even + sink_of(2 * i))
            odd = odd / (pltpu.roll(odd, HEAD_DIM, 1) + sink_of(2 * i + 1))
            ctx[t, i] = jnp.where(low, even, odd).astype(BF16)
            if ends:

                @pl.when((yh == 1) & (x + k * (NX // 4) < NX // 2) & jnp.logical_not(middle))
                def _(i=i):
                    around_out(i).start()

            for dt in (2, 1, 3)[: NT - 1] if ends else range(1, NT):

                @pl.when(direct(dt))
                def _(i=i, dt=dt):
                    ctx_copy(i, dt).start()

        return 0

    lax.fori_loop(0, 2, finish_stack, 0)
    pl.when(early)(o_take)

    def project(tt):
        total = None
        for i in range(0, PAIRS, 2):
            role = tt * (R // NT) + i
            rows = jnp.concatenate([wo_all[role], wo_all[role + 1]], axis=1)
            heads = jnp.concatenate([ctx[tt, i], ctx[tt, i + 1]], axis=1)
            part = lax.dot_general(
                rows, heads, (((1,), (1,)), ((), ())), preferred_element_type=F32
            )
            total = part if total is None else total + part
        return total

    if ends:

        @pl.when(middle)
        def _():
            def relay(i):
                ctx_copy(i, 2).wait_recv()
                ctx_pass(i, 1).start()

            for i in range(PAIRS):
                ctx_copy(i, jnp.where(t == 1, 3, 1)).wait_recv()
                ctx_pass(i, 0).start()
                pl.when((yh == 0) | jnp.logical_not(rounds(i)))(functools.partial(relay, i))

            for i in range(PAIRS):

                @pl.when((yh == 0) & rounds(i))
                def _(i=i):
                    around_out(i).wait_recv()
                    around_on(i).start()

    o_take_far(1)
    for dy in range(2):
        for dx in range(NX):
            o_twin(dy, dx).wait_recv()
    out_acc[...] = project(t)
    for k in range(1, NT):
        source = lax.rem(t + k, NT)
        if ends:
            order = ((1, 2, 3), (0, 2, 3), (1, 3, 0), (2, 1, 0))
            source = order[3][k - 1]
            for where in range(3):
                source = jnp.where(t == where, order[where][k - 1], source)
        dt = lax.rem(t + NT - source, NT)
        for i in range(PAIRS):
            waited = (t < 0) | (t > NT)
            if ends:
                passed = (dt == 2) & ((yh == 0) | jnp.logical_not(rounds(i)))
                waited = middle & ((source == 1) | (source == 2) | passed)

            @pl.when(jnp.logical_not(waited))
            def _(i=i, dt=dt):
                ctx_copy(i, dt).wait_recv()

        out_acc[...] += project(source)
    out[...] = out_acc[...].astype(BF16)

    for copy in [w_across, o_across] + w_far + w_beyond:
        copy.wait_send()
    for dy in range(2):
        for i in range(len(near)):
            o_side(dy, i).wait_send()
            if far:
                o_on(dy, i).wait_send()
        for dx in range(NX):
            o_twin(dy, dx).wait_send()

    @pl.when(yh == 0)
    def _():
        gather_k.across().wait_send()

    for dx in range(NX):

        @pl.when((x + dx < NX) & (dx > 0))
        def _(dx=dx):
            gather_k.along(dx).wait_send()

        @pl.when(x >= dx)
        def _(dx=dx):
            gather_k.twin_near(dx).wait_send()


    @pl.when(yh == 1)
    def _():
        for dx in offsets:
            gather_k.along_other(dx).wait_send()
        for dx in range(NX):
            gather_k.twin_other(dx).wait_send()

    for j in travels:
        for s in range(1, H + 1):
            for d in ways(s, j):
                ring(d, s, j).wait_send()
    for s in range(H + 1):
        for d in both(s):
            for copy in sides(d, s) + [twin_plane(d, s)]:
                copy.wait_send()
    for i in range(PAIRS):
        for dt in range(1, NT):

            @pl.when(direct(dt))
            def _(i=i, dt=dt):
                ctx_copy(i, dt).wait_send()

    if ends:

        @pl.when(middle)
        def _():
            for i in range(PAIRS):
                ctx_pass(i, 0).wait_send()
                pl.when((yh == 0) | jnp.logical_not(rounds(i)))(ctx_pass(i, 1).wait_send)
                pl.when((yh == 0) & rounds(i))(around_on(i).wait_send)

        for i in range(PAIRS):

            @pl.when((yh == 1) & rounds(i) & jnp.logical_not(middle))
            def _(i=i):
                around_out(i).wait_send()


def rotation_tables(rows, roles):
    half = HEAD_DIM // 2
    freq = np.exp(-math.log(150000.0) * np.arange(half) / half)
    freq = np.tile(freq, 128 // half)[None, :]
    near = np.arange(rows)[:, None] * freq
    far = (np.arange(roles) * rows)[:, None] * freq
    return [a.astype(np.float32) for a in (np.cos(near), np.sin(near), np.cos(far), np.sin(far))]


def on_device(sizes, tokens, gain, q_weight, kv_weight, out_weight, sinks, segments):
    NG, NT, R = sizes
    feature = tokens[0].T
    width, rows = feature.shape
    NX = R // 4
    heads = q_weight.shape[1] // HEAD_DIM
    columns = q_weight.shape[1] + kv_weight.shape[1]
    features_out = out_weight.shape[1]
    tables = [jnp.asarray(a) for a in rotation_tables(rows, R)]
    H = NG // 2
    dims = (NG, NT, R, NX, rows, width)
    vmem = pl.BlockSpec(memory_space=pltpu.VMEM)
    anywhere = pl.BlockSpec(memory_space=pl.ANY)
    dma = pltpu.SemaphoreType.DMA
    out = pl.pallas_call(
        functools.partial(kernel, dims),
        out_shape=jax.ShapeDtypeStruct((features_out, rows), BF16),
        in_specs=[anywhere, vmem, vmem, vmem, anywhere, vmem]
        + [pl.BlockSpec(memory_space=pltpu.SMEM)]
        + [vmem] * 4,
        out_specs=vmem,
        scratch_shapes=[
            pltpu.VMEM((width, rows), BF16),
            pltpu.VMEM((width, rows), BF16),
            pltpu.VMEM((NG, rows, R * 16), BF16),
            pltpu.VMEM((16, columns), BF16),
            pltpu.VMEM((NG, R, 16, columns), BF16),
            pltpu.VMEM((rows, columns), F32),
            pltpu.VMEM((heads, rows, 128), BF16),
            pltpu.VMEM((R, rows + 16, 128), BF16),
            pltpu.VMEM((R, rows, 128), BF16),
            pltpu.VMEM((rows, 128), F32),
            pltpu.VMEM((R, rows, rows), F32),
            pltpu.VMEM((heads, rows, 128), F32),
            pltpu.VMEM((R, features_out, 128), BF16),
            pltpu.VMEM((NT, heads // 2, rows, 128), BF16),
            pltpu.VMEM((heads // 2, rows, 128), BF16),
            pltpu.VMEM((features_out, rows), F32),
            dma((2,)),
            dma((3, 9 + 2 * NX)),
            dma((3, 9 + 2 * NX)),
            dma((2, H, R // 2)),
            dma((2, H, R // 2)),
            dma((2, H + 1, 4)),
            dma((2, H + 1, 4)),
            dma((2, H + 1)),
            dma((2, H + 1)),
            dma((heads // 2, NT)),
            dma((heads // 2, NT)),
            dma((2, heads // 2)),
            dma((2, heads // 2)),
            dma((heads // 2,)),
        ],
        compiler_params=pltpu.CompilerParams(collective_id=0, has_side_effects=True),
        name="layer",
    )(
        feature,
        gain,
        q_weight,
        kv_weight,
        out_weight.T,
        segments,
        sinks,
        *tables,
    )
    return out.T[None]


def solution(mesh):
    placed = (
        P("group", "role", None),
        P(),
        P(("group", "role"), "tensor"),
        P(("group", "role"), "tensor"),
        P("role", "tensor"),
        P("tensor"),
        P("group", "role"),
    )
    sizes = (mesh.shape["group"], mesh.shape["tensor"], mesh.shape["role"])
    return jax.shard_map(
        functools.partial(on_device, sizes),
        mesh=mesh,
        in_specs=placed,
        out_specs=P("group", "role", "tensor"),
        check_vma=False,
    )
```
